32 devices in a mesh: space: 16 (over z, y, x), rep: 2 (over core).
Axes of the slice: x: 2, y: 2, z: 4, core: 2. Of those that a mesh axis runs over, the one named last changes fastest.
Arguments:
- halo_rows: bfloat16 [4, 2048, 256], P(None, 'space', 'rep'), may hold values from -6 to 6
- unmatched: int32 [4, 2048], P(None, 'space'), may hold values 0 or 1
- owner_id: int32 [4, 2048, 1], P(None, 'space'), may hold values from 0 to 15; in each aligned block of 128 rows (0 to 127, 128 to 255, ..., all dimensions but the last counted through in order) at most 16 rows name the same one
- cand_index: int32 [4, 2048, 16], P(None, 'space'), may hold values from 0 to 511
- lengths: int32 [4, 2048], P(None, 'space'), may hold values from 1 to 16
- choice_index: int32 [4, 2048], P(None, 'space'), may hold values from 0 to 15, as said below
- desc_rows: bfloat16 [4, 8192, 256], P(None, 'space', 'rep'), may hold values from -6 to 6
Outputs:
- phantom: bfloat16 [4, 2048, 256], P(None, 'space', 'rep')
- best_merit: bfloat16 [4, 2048], P(None, 'space')
The draws below stay inside these ranges and needn't reach their ends.
Inputs may be any that keep to these rules, and one draw needn't show every extreme that they name: `owner_id`: in each aligned block of 128 halos (one region in one snapshot) no owner is named by more than 16 halos, a bound that some block reaches. `choice_index`: less than the halo's length.
All inputs are finite; a program needn't handle non-finite values. No bound on the sum of `unmatched` on one device may be relied on, other than what follows from the above.
Results may differ from the reference program's by a relative error of at most 0.001.
Values may be sent and summed in bfloat16 or wider, within the bound.
A program may use at most 64 MiB of HBM per device.

```python
import math
import jax
import jax.numpy as jnp
import numpy as np
from jax import lax

WIDTH = 256
SNAPS = 4
K = 16
HALO_DEV = 128
CAND_DEV = 512
CAP = 16
HALOS = 2048
CANDS = 8192
N_SPACE = 16


def draw_pair(key):
    base_key = jax.random.fold_in(key, 71)
    first_key, second_key = jax.random.split(base_key)
    span_draw = jax.random.randint(first_key, (SNAPS, HALOS), 1, K + 1)
    pick_draw = jax.random.randint(second_key, (SNAPS, HALOS), 0, 1048576) % span_draw
    return (span_draw, pick_draw)


def draw_lengths(key, part):
    return draw_pair(key)[0].astype(jnp.int32)


def draw_choice_index(key, part):
    return draw_pair(key)[1].astype(jnp.int32)


def place_ends(values, rng, smallest, top_value):
    shape = values.shape
    index_at = [jax.random.randint(jax.random.fold_in(rng, axis), (), 0, shape[axis]) for axis in range(len(shape))]
    values = values.at[tuple(index_at)].set(smallest)
    longest = shape.index(max(shape))
    index_at[longest] = (index_at[longest] + 1) % shape[longest]
    return values.at[tuple(index_at)].set(top_value)


def shard_levels(stream_key, extent, shards, low, largest):
    level, own = 1.0, jax.random.fold_in(stream_key, 6)
    for position, parts in shards:
        draws = jnp.exp(jax.random.uniform(jax.random.fold_in(own, position), (parts,), jnp.float32, low / len(shards), largest / len(shards)))
        level = level * jnp.repeat(draws, extent[position] // parts).reshape([-1 if axis == position else 1 for axis in range(len(extent))])
    return level


def routed_block(own_key, own, number, rows, count, top, limit, skew):
    order = jax.random.permutation(own_key, count)
    packed, common = shares(count, rows * top, limit, skew, True), shares(count, rows * top, limit, skew, False)
    places = jnp.arange(count)

    def named(tallies, offset_by):
        used = int((tallies > 0).sum())
        fixed = max(1, used // 4)
        passed = fixed + (places - fixed + offset_by * (used - fixed)) % max(1, count - fixed)
        return jnp.zeros((count,), jnp.int32).at[order[jnp.where(places < fixed, places, passed)]].set(jnp.asarray(tallies, jnp.int32))

    tallies = jnp.where(number % 4 == 0, named(packed, number // 4), named(common, number - number // 4 - 1))
    mixed = jax.random.permutation(jax.random.fold_in(own, 3), count)
    giver, receiver = mixed[0:count // 2 * 2:2], mixed[1:count // 2 * 2:2]
    room = jnp.minimum(tallies[giver] - 1, limit - tallies[receiver]) // 2
    room = jnp.where((giver == order[0]) | (receiver == order[0]) | (tallies[receiver] == 0), 0, jnp.maximum(room, 0))
    passed = jax.random.randint(jax.random.fold_in(own, 4), (count // 2,), 0, 1 << 20) % (room + 1)
    tallies = tallies.at[giver].add(-passed).at[receiver].add(passed)
    items = jnp.searchsorted(jnp.cumsum(tallies), jnp.arange(rows * top), side="right").astype(jnp.int32)
    grid = items.reshape(top, rows).T
    grid = grid[jax.random.permutation(jax.random.fold_in(own, 1), rows)]
    offset_by = jax.random.randint(jax.random.fold_in(own, 2), (rows, 1), 0, top)
    return jnp.take_along_axis(grid, (jnp.arange(top)[None, :] + offset_by) % top, axis=1)


def shares(amount, total, limit, slope, full):
    portions = [(1 << 20) // math.isqrt(rank ** slope) + 1 for rank in range(1, amount + 1)]
    largest = limit if full else min(limit, max(-(-total // amount), total * portions[0] // sum(portions)))
    least = 1 if total - largest >= amount - 1 else 0
    counts, rest = [largest] + [least] * (amount - 1), total - largest - least * (amount - 1)
    while rest > 0:
        movable = [i for i in range(1, amount) if counts[i] < largest] or [i for i in range(1, amount) if counts[i] < limit]
        pool, budget = sum([portions[i] for i in movable]), rest
        for i in movable:
            extra = min(limit - counts[i], max(1, budget * portions[i] // pool), rest)
            counts[i] = counts[i] + extra
            rest = rest - extra
    return np.array(counts)


def noise(own_key, dims, deviation, bound, shards=(), kind=jnp.bfloat16):
    entries = jax.random.normal(own_key, dims, jnp.float32) * deviation
    if len(shards) > 0:
        entries = shard_levels(own_key, dims, shards, -0.22, 0.18) * entries
    return jnp.clip(entries, min=-bound, max=bound).astype(kind)


def setup_inputs(seed: int = 0) -> dict:
    splits = jax.random.split(jax.random.key(seed), 8)
    halo_rows = noise(splits[0], (SNAPS, HALOS, WIDTH), 1.0, 6.0, ((1, 16), (2, 2)))
    unmatched = place_ends((jax.random.randint(splits[1], (SNAPS, HALOS), 0, 3) < 2).astype(jnp.int32), jax.random.fold_in(splits[1], 1), 0, 1)
    owner_id_keys = jax.random.split(jax.random.fold_in(splits[2], 1), SNAPS * HALOS // HALO_DEV)
    owner_id_turns = jax.random.permutation(jax.random.fold_in(splits[2], 3), SNAPS * HALOS // HALO_DEV)
    owner_id = jax.vmap(lambda own, number: routed_block(jax.random.fold_in(splits[2], 2), own, number, HALO_DEV, N_SPACE, 1, CAP, 2))(owner_id_keys, owner_id_turns).reshape((SNAPS, HALOS, 1))
    cand_index = place_ends(jax.random.randint(splits[3], (SNAPS, HALOS, K), 0, CAND_DEV), jax.random.fold_in(splits[3], 1), 0, CAND_DEV - 1).astype(jnp.int32)
    lengths = draw_lengths(jax.random.fold_in(splits[7], 71), 0)
    choice_index = draw_choice_index(jax.random.fold_in(splits[7], 71), 0)
    desc_rows = noise(splits[6], (SNAPS, CANDS, WIDTH), 1.0, 6.0, ((1, 16), (2, 2)))
    return dict(halo_rows=halo_rows, unmatched=unmatched, owner_id=owner_id, cand_index=cand_index, lengths=lengths, choice_index=choice_index, desc_rows=desc_rows)


def reference(halo_rows, unmatched, owner_id, cand_index, lengths, choice_index, desc_rows):
    phantom_list = []
    best_list = []
    lane_ids = jnp.arange(K, dtype=jnp.int32)
    block_size = math.gcd(HALOS, 4096)
    for snapshot in range(SNAPS):
        rows_here = halo_rows[snapshot]
        desc_table = desc_rows[snapshot]
        glob = (owner_id[snapshot, :, 0][:, None] * CAND_DEV + cand_index[snapshot]).astype(jnp.int32)

        def score_block(pieces):
            rows_block, glob_block = pieces
            picked = desc_table[glob_block].astype(jnp.float32)
            return jnp.einsum('rkw,rw->rk', picked, rows_block.astype(jnp.float32))
        merit_full = lax.map(score_block, (rows_here.reshape(-1, block_size, WIDTH), glob.reshape(-1, block_size, K)))
        merit_full = merit_full.reshape(HALOS, K) / math.sqrt(WIDTH)
        live_halo = unmatched[snapshot] == 1
        used = lane_ids[None, :] < lengths[snapshot][:, None]
        live_entry = used & live_halo[:, None]
        quality = 1.0 + jax.nn.softplus(merit_full)
        claims = jnp.zeros((CANDS,), jnp.float32).at[glob.reshape(-1)].max(jnp.where(live_entry, quality, jnp.zeros_like(quality)).reshape(-1))
        pick_pos = choice_index[snapshot][:, None].astype(jnp.int32)
        chosen = jnp.take_along_axis(glob, pick_pos, 1)[:, 0]
        chosen_quality = jnp.take_along_axis(quality, pick_pos, 1)[:, 0]
        share_weight = chosen_quality / (chosen_quality + claims[chosen])
        blended = ((1.0 - share_weight)[:, None] * rows_here.astype(jnp.float32) + share_weight[:, None] * desc_table[chosen].astype(jnp.float32)).astype(jnp.bfloat16)
        phantom_list.append(jnp.where(live_halo[:, None], blended, rows_here))
        top_merit = lax.optimization_barrier(jnp.max(jnp.where(used, merit_full, jnp.full_like(merit_full, -1e+30)), axis=1))
        best_list.append(jnp.where(live_halo, top_merit, jnp.zeros_like(top_merit)).astype(jnp.bfloat16))
    return (jnp.stack(phantom_list), jnp.stack(best_list))
```

```python
import functools
import math

import jax
import jax.numpy as jnp
from jax import lax
from jax.experimental import pallas as pl
from jax.experimental.pallas import tpu as pltpu
from jax.sharding import PartitionSpec as P

MESH = pl.DeviceIdType.MESH
F32 = jnp.float32
BF16 = jnp.bfloat16
NEG = -1e30
GROUP = 32
NT = (((1,), (1,)), ((), ()))


def iota(shape, dim):
    return lax.broadcasted_iota(jnp.int32, shape, dim)


def dot(a, b):
    return jnp.dot(a, b, preferred_element_type=F32)


def dot_nt(a, b):
    return lax.dot_general(a, b, NT, preferred_element_type=F32)


def hot(mask):
    return jnp.where(mask, 1.0, 0.0).astype(BF16)


def code(index, cands):
    return index - cands // 2 + jnp.where(index >= cands // 2, 1, 0)


def kernel(
    n, slots, width,
    halo_in, unmatched_in, owner_in, cand_in, lengths_in, choice_in, desc_in,
    phantom, best,
    halo, unmatched, owner, cand, lengths, choice, desc, table,
    send, recv, send_meta, recv_meta, scores, bias, pick, recv_pick, res, recv_res,
    row_sem, meta_sem, pick_ss, pick_rs, res_ss, res_rs, table_sem, load_sem,
):
    me, core = lax.axis_index("space"), lax.axis_index("rep")
    snaps, halos, half = halo.shape
    k_count = cand.shape[1]
    cands = desc.shape[1]
    own = snaps // 2
    total = n * slots
    hs = slots // 2

    def core_of(x):
        return lax.rem(core + x, 2)

    def remote(src, dst, ss, rs, peer, x):
        return pltpu.make_async_remote_copy(
            src_ref=src, dst_ref=dst, send_sem=ss, recv_sem=rs,
            device_id=(peer, core_of(x)), device_id_type=MESH,
        )

    def whole(ref, ss, rs):
        return remote(ref, ref, ss, rs, me, 1)

    def each_chip(f):
        @pl.loop(1, n)
        def _(d):
            f(lax.rem(me + d, n))

    def each_peer(f):
        def both(peer):
            f(peer, 0)
            f(peer, 1)

        each_chip(both)
        f(me, 1)

    barrier = pltpu.get_barrier_semaphore()
    each_peer(
        lambda peer, x: pl.semaphore_signal(
            barrier, inc=1, device_id=(peer, core_of(x)), device_id_type=MESH
        ),
    )
    loads = [
        pltpu.make_async_copy(src, dst, load_sem.at[i])
        for i, (src, dst) in enumerate(
            [
                (owner_in, owner), (unmatched_in, unmatched), (cand_in, cand),
                (lengths_in, lengths), (choice_in, choice), (halo_in, halo), (desc_in, desc),
            ]
        )
    ]
    for load in loads:
        load.start()
    for load in loads[:5]:
        load.wait()

    order = [(x, ls) for x in range(2) for ls in range(own)]
    named = [iota((n, halos), 0) == owner[own * core_of(x) + ls] for x, ls in order]
    onehot = hot(jnp.concatenate(named, axis=0))
    before = dot(onehot, hot(iota((halos, halos), 0) < iota((halos, halos), 1)))
    route = []
    for i, (x, ls) in enumerate(order):
        s = own * core_of(x) + ls
        rank = jnp.sum(
            jnp.where(named[i], before[i * n : (i + 1) * n], 0.0), axis=0, keepdims=True
        ).astype(jnp.int32)
        live = unmatched[pl.ds(s, 1), :] == 1
        dest = owner[s]
        route.append((dest, rank, jnp.where(live, dest * slots + rank, -1), live))

    blocks, rows = [], []
    for i, (x, ls) in enumerate(order):
        s = own * core_of(x) + ls
        dest, rank, _, live = route[i]
        listed = code(cand[s], cands)
        k_ids = iota((k_count, halos), 0)
        taken = jnp.sum(jnp.where(k_ids == choice[pl.ds(s, 1), :], listed, 0), axis=0, keepdims=True)
        taken = jnp.broadcast_to(taken, (8, halos))
        none = jnp.zeros((8, halos), jnp.int32)
        if x == 0:
            listed = jnp.where(k_ids < lengths[pl.ds(s, 1), :], listed, 0)
            parts = [listed, taken, none]
        else:
            parts = [jnp.zeros((k_count, halos), jnp.int32), none, taken]
        parts = [jnp.zeros((GROUP * ls, halos), jnp.int32)] * (ls > 0) + parts
        if ls < own - 1:
            parts.append(jnp.zeros((GROUP * (own - 1 - ls), halos), jnp.int32))
        blocks.append(jnp.concatenate(parts, axis=0).astype(F32).astype(BF16))
        rows.append(
            [
                jnp.where(live & (rank >= g * hs) & (rank < (g + 1) * hs), dest * hs + rank - g * hs, -1)
                for g in range(2)
            ]
        )
    block = jnp.concatenate(blocks, axis=1)
    blank = jnp.zeros_like(block)
    meta = sum(
        dot_nt(
            jnp.concatenate([hot(iota((n * hs, halos), 0) == r[g]) for r in rows], axis=1),
            jnp.concatenate([blank, block] if g else [block, blank], axis=0),
        )
        for g in range(2)
    )
    send_meta[...] = meta.astype(BF16).reshape(n, hs, 128)

    loads[5].wait()
    for i, (x, ls) in enumerate(order):
        place = hot(iota((total, halos), 0) == route[i][2])
        packed = dot(place, halo[own * core_of(x) + ls]).astype(BF16)
        send[x * n : (x + 1) * n, ls] = packed.reshape(n, slots, half)

    pl.semaphore_wait(barrier, 2 * n - 1)

    each_chip(
        lambda peer: remote(
            send_meta.at[peer], recv_meta.at[me], meta_sem.at[0], meta_sem.at[1], peer, 0
        ).start()
    )
    each_peer(
        lambda peer, x: remote(
            send.at[x * n + peer], recv.at[x * n + me], row_sem.at[0], row_sem.at[1], peer, x
        ).start()
    )
    table_copy = remote(
        desc_in.at[pl.ds(own * core_of(1), own)], table, table_sem.at[0], table_sem.at[1], me, 1
    )
    table_copy.start()
    recv_meta[me] = send_meta[me]
    recv[me] = send[me]

    lines = [v.astype(F32) for dest, rank, target, live in route for v in (dest, jnp.where(live, rank, -halos), target)]
    lines = jnp.concatenate(lines + [jnp.zeros((128 - len(lines), halos), F32)], axis=0).T
    back = []
    lane = iota((halos, 128), 1).astype(F32)
    for i in range(snaps):
        dest, rank, target = [lines[:, 3 * i + j : 3 * i + j + 1] for j in range(3)]
        back.append(
            (
                hot(iota((halos, n), 1).astype(F32) == dest),
                (lane == rank) | (lane == rank + slots),
                lane == rank + 2 * slots,
                hot(iota((halos, total), 1).astype(F32) == target),
            )
        )
    entry = iota((n * hs, total), 0)
    column = iota((n * hs, total), 1)
    inside = column % slots
    unpack = [
        hot((entry == (column // slots) * hs + inside - g * hs) & (inside // hs == g)) for g in range(2)
    ]
    loads[6].wait()

    whole(recv_meta.at[pl.ds(0, n - 1)], meta_sem.at[0], meta_sem.at[1]).wait_recv()
    arrived = recv_meta[...].reshape(n * hs, 128).astype(F32)
    ids = code(iota((n * hs, cands), 1), cands).astype(F32)
    for ls in range(own):
        for x in range(2):
            lanes = [(g * own + ls) * GROUP + k_count + 8 * x for g in range(2)]
            select = jnp.concatenate([hot(arrived[:, at : at + 1] == ids) for at in lanes], axis=0)
            chosen = dot(select, desc[own * core_of(x) + ls]).astype(BF16)
            for g in range(2):
                pick[ls, :, x, g * hs : (g + 1) * hs, :] = chosen[
                    g * n * hs : (g + 1) * n * hs
                ].reshape(n, hs, half)
        each_chip(
            lambda peer: remote(
                pick.at[ls, peer], recv_pick.at[ls, me], pick_ss.at[ls], pick_rs.at[ls], peer, 0
            ).start()
        )
        recv_pick[ls, me] = pick[ls, me]

    step = 64
    arrived = arrived.T.astype(BF16)
    picks = []
    for ls in range(own):
        lists = sum(
            dot(arrived[(g * own + ls) * GROUP : (g * own + ls + 1) * GROUP], unpack[g]) for g in range(2)
        )
        picks.append(lists[k_count : k_count + 1])

        @pl.loop(0, cands // step)
        def _(i):
            ids = code(iota((step, total), 0) + i * step, cands).astype(F32)
            mask = ids == lists[0:1]
            for k in range(1, k_count):
                mask = mask | (ids == lists[k : k + 1])
            bias[ls, pl.ds(pl.multiple_of(i * step, step), step), :] = jnp.where(mask, 0.0, NEG)

    scale = 1.0 / math.sqrt(width)
    owned = iota((n, total), 0) == iota((n, total), 1) // slots
    fold = jnp.concatenate(
        [hot(iota((total, 128), 1) == part * slots + iota((total, 128), 0) % slots) for part in range(3)],
        axis=0,
    )

    table_copy.wait_recv()
    whole(recv.at[pl.ds(0, 2 * n - 1)], row_sem.at[0], row_sem.at[1]).wait_recv()
    for ls in range(own):
        scores[...] = dot_nt(
            jnp.concatenate([desc[own * core + ls], table[ls]], axis=1),
            jnp.concatenate(
                [recv[x * n : (x + 1) * n, ls].reshape(total, half) for x in range(2)], axis=1
            ),
        )

        def chunk(i, carry):
            top, picked, claimed = carry
            at = pl.ds(pl.multiple_of(i * step, step), step)
            value = scores[at, :]
            masked = value + bias[ls, at, :]
            claim = jnp.max(masked, axis=1, keepdims=True)
            chosen = code(iota((step, total), 0) + i * step, cands).astype(F32) == picks[ls]

            def least(v):
                return jnp.max(v.reshape(step // 8, 8, total), axis=0)

            return (
                jnp.maximum(top, least(masked)),
                jnp.maximum(picked, least(jnp.where(chosen, value, NEG))),
                jnp.maximum(claimed, least(jnp.where(chosen, claim, NEG))),
            )

        start = jnp.full((8, total), NEG, F32)
        top, picked, claimed = [
            jnp.max(v, axis=0, keepdims=True)
            for v in lax.fori_loop(0, cands // step, chunk, (start, start, start))
        ]

        def quality(v):
            v = v * scale
            return 1.0 + jnp.maximum(v, 0.0) + jnp.log(1.0 + jnp.exp(-jnp.abs(v)))

        mine = quality(picked)
        share = mine / (mine + quality(claimed))
        high = share.astype(BF16).astype(F32)
        top = jnp.where(top > NEG * 0.5, top * scale, 0.0)
        spread = jnp.concatenate(
            [jnp.where(owned, jnp.broadcast_to(v, (n, total)), 0.0) for v in (high, share - high, top)],
            axis=1,
        ).astype(BF16)
        res[ls] = dot(spread, fold).reshape(n, 1, 128)
        each_peer(
            lambda peer, x: remote(
                res.at[ls, peer], recv_res.at[ls, x * n + me], res_ss.at[ls], res_rs.at[ls], peer, x
            ).start()
        )
        recv_res[ls, me] = res[ls, me]

    ones = jnp.ones((128, half), BF16)
    tops = []
    for ls in range(own):
        whole(recv_pick.at[ls, pl.ds(0, n - 1)], pick_ss.at[ls], pick_rs.at[ls]).wait_recv()
        rows = [
            dot(back[x * own + ls][3], recv_pick[ls, :, x].reshape(total, half)) for x in range(2)
        ]
        whole(recv_res.at[ls, pl.ds(0, 2 * n - 1)], res_ss.at[ls], res_rs.at[ls]).wait_recv()
        for x in range(2):
            s = own * core_of(x) + ls
            named, shared, topped, _ = back[x * own + ls]
            brought = recv_res[ls, x * n : (x + 1) * n].reshape(n, 128).astype(BF16)
            spread = dot(named, brought)
            share = dot(jnp.where(shared, spread, 0.0).astype(BF16), ones)
            phantom[s] = ((1.0 - share) * halo[s].astype(F32) + share * rows[x]).astype(BF16)
            tops.append(dot_nt(ones[0:8], jnp.where(topped, spread, 0.0).astype(BF16))[0:1])
    first, second = jnp.concatenate(tops[0::2], axis=0), jnp.concatenate(tops[1::2], axis=0)
    even = core == 0
    best[...] = jnp.concatenate(
        [jnp.where(even, first, second), jnp.where(even, second, first)], axis=0
    ).astype(BF16)

    table_copy.wait_send()
    whole(send_meta.at[pl.ds(0, n - 1)], meta_sem.at[0], meta_sem.at[1]).wait_send()
    whole(send.at[pl.ds(0, 2 * n - 1)], row_sem.at[0], row_sem.at[1]).wait_send()
    for ls in range(own):
        whole(pick.at[ls, pl.ds(0, n - 1)], pick_ss.at[ls], pick_rs.at[ls]).wait_send()
        whole(recv_res.at[ls, pl.ds(0, 2 * n - 1)], res_ss.at[ls], res_rs.at[ls]).wait_send()


def hand_over(phantom_in, best_in, phantom, best):
    phantom[...] = phantom_in[...]
    best[...] = best_in[...]


def body(n, halo_rows, unmatched, owner_id, cand_index, lengths, choice_index, desc_rows):
    snaps, halos, half = halo_rows.shape
    cands = desc_rows.shape[1]
    own = snaps // 2
    slots = max(2 * halos // n, 16)
    total = n * slots
    dma = pltpu.SemaphoreType.DMA
    results = pl.pallas_call(
        functools.partial(kernel, n, slots, 2 * half),
        out_shape=(
            pltpu.VMEM((snaps, halos, half), BF16),
            pltpu.VMEM((snaps, halos), BF16),
        ),
        in_specs=[pl.BlockSpec(memory_space=pl.ANY)] * 7,
        out_specs=(pl.BlockSpec(memory_space=pltpu.VMEM),) * 2,
        scratch_shapes=[
            pltpu.VMEM(halo_rows.shape, BF16),
            pltpu.VMEM(unmatched.shape, jnp.int32),
            pltpu.VMEM((snaps, 1, halos), jnp.int32),
            pltpu.VMEM((snaps, cand_index.shape[2], halos), jnp.int32),
            pltpu.VMEM(lengths.shape, jnp.int32),
            pltpu.VMEM(choice_index.shape, jnp.int32),
            pltpu.VMEM((snaps, cands, half), BF16),
            pltpu.VMEM((own, cands, half), BF16),
            pltpu.VMEM((2 * n, own, slots, half), BF16),
            pltpu.VMEM((2 * n, own, slots, half), BF16),
            pltpu.VMEM((n, slots // 2, 128), BF16),
            pltpu.VMEM((n, slots // 2, 128), BF16),
            pltpu.VMEM((cands, total), F32),
            pltpu.VMEM((own, cands, total), F32),
            pltpu.VMEM((own, n, 2, slots, half), BF16),
            pltpu.VMEM((own, n, 2, slots, half), BF16),
            pltpu.VMEM((own, n, 1, 128), F32),
            pltpu.VMEM((own, 2 * n, 1, 128), F32),
            dma((2,)), dma((2,)), dma((own,)), dma((own,)), dma((own,)), dma((own,)), dma((2,)), dma((7,)),
        ],
        compiler_params=pltpu.CompilerParams(collective_id=0, has_side_effects=True),
    )(
        halo_rows,
        unmatched,
        jnp.swapaxes(owner_id, 1, 2),
        jnp.swapaxes(cand_index, 1, 2),
        lengths,
        choice_index,
        desc_rows,
    )
    shapes = tuple(jax.ShapeDtypeStruct(v.shape, v.dtype) for v in results)
    return pl.pallas_call(
        hand_over,
        out_shape=shapes,
        in_specs=[pl.BlockSpec(memory_space=pltpu.VMEM)] * 2,
        out_specs=(pl.BlockSpec(memory_space=pltpu.VMEM),) * 2,
    )(*[pltpu.with_memory_space_constraint(v, pltpu.VMEM) for v in results])


def solution(mesh):
    in_specs = (
        P(None, "space", "rep"),
        P(None, "space"),
        P(None, "space", None),
        P(None, "space", None),
        P(None, "space"),
        P(None, "space"),
        P(None, "space", "rep"),
    )
    out_specs = (P(None, "space", "rep"), P(None, "space"))
    return jax.shard_map(
        functools.partial(body, mesh.shape["space"]),
        mesh=mesh, in_specs=in_specs, out_specs=out_specs, check_vma=False,
    )
```

```python
import functools
import math

import jax
import jax.numpy as jnp
from jax import lax
from jax.experimental import pallas as pl
from jax.experimental.pallas import tpu as pltpu
from jax.sharding import PartitionSpec as P

MESH = pl.DeviceIdType.MESH
F32 = jnp.float32
BF16 = jnp.bfloat16
NEG = -1e30
GROUP = 32
NT = (((1,), (1,)), ((), ()))


def iota(shape, dim):
    return lax.broadcasted_iota(jnp.int32, shape, dim)


def dot(a, b):
    return jnp.dot(a, b, preferred_element_type=F32)


def dot_nt(a, b):
    return lax.dot_general(a, b, NT, preferred_element_type=F32)


def hot(mask):
    return jnp.where(mask, 1.0, 0.0).astype(BF16)


def code(index, cands):
    return index - cands // 2 + jnp.where(index >= cands // 2, 1, 0)


def kernel(
    n, slots, width,
    halo_in, unmatched_in, owner_in, cand_in, lengths_in, choice_in, desc_in,
    phantom, best,
    halo, unmatched, owner, cand, lengths, choice, desc, table,
    send, recv, send_want, recv_want, send_meta, recv_meta, scores, bias, pick, recv_pick, res, recv_res,
    row_sem, want_sem, meta_sem, pick_sem, res_sem, table_sem, load_sem,
):
    me, core = lax.axis_index("space"), lax.axis_index("rep")
    snaps, halos, half = halo.shape
    k_count = cand.shape[1]
    cands = desc.shape[1]
    own = snaps // 2
    total = n * slots
    hs = slots // 2

    def core_of(x):
        return 1 - core if x else core

    def remote(src, dst, ss, rs, peer, x):
        return pltpu.make_async_remote_copy(
            src_ref=src, dst_ref=dst, send_sem=ss, recv_sem=rs,
            device_id=(peer, core_of(x)), device_id_type=MESH,
        )

    def whole(ref, ss, rs):
        return remote(ref, ref, ss, rs, me, 1)

    def each_chip(f):
        if n % 4 or n > 32:

            @pl.loop(1, n)
            def _(d):
                peer = me + d
                f(jnp.where(peer >= n, peer - n, peer))

            return
        block, place = me // 4, lax.rem(me, 4)
        for d in [*range(1, n // 4), 0]:
            to = block + d
            to = jnp.where(to >= n // 4, to - n // 4, to) * 4
            for q in (3, 1, 2, 0):
                if d or q:
                    f(to + jnp.bitwise_xor(place, q))

    def each_peer(f):
        def both(peer):
            f(peer, 0)
            f(peer, 1)

        each_chip(both)
        f(me, 1)

    barrier = pltpu.get_barrier_semaphore()
    each_peer(
        lambda peer, x: pl.semaphore_signal(
            barrier, inc=1, device_id=(peer, core_of(x)), device_id_type=MESH
        ),
    )
    loads = [
        pltpu.make_async_copy(src, dst, load_sem.at[i])
        for i, (src, dst) in enumerate(
            [
                (owner_in, owner), (unmatched_in, unmatched), (cand_in, cand),
                (lengths_in, lengths), (choice_in, choice), (halo_in, halo), (desc_in, desc),
            ]
        )
    ]
    for load in loads:
        load.start()
    for load in loads[:5]:
        load.wait()

    order = [(x, ls) for x in range(2) for ls in range(own)]
    named = [iota((n, halos), 0) == owner[own * core_of(x) + ls] for x, ls in order]
    onehot = hot(jnp.concatenate(named, axis=0))
    before = dot(onehot, hot(iota((halos, halos), 0) < iota((halos, halos), 1)))
    route = []
    for i, (x, ls) in enumerate(order):
        s = own * core_of(x) + ls
        rank = jnp.sum(
            jnp.where(named[i], before[i * n : (i + 1) * n], 0.0), axis=0, keepdims=True
        ).astype(jnp.int32)
        live = unmatched[pl.ds(s, 1), :] == 1
        dest = owner[s]
        route.append((dest, rank, jnp.where(live, dest * slots + rank, -1), live))

    k_ids = iota((k_count, halos), 0)
    wants, coded = [], []
    for i, (x, ls) in enumerate(order):
        s = own * core_of(x) + ls
        _, rank, _, live = route[i]
        coded.append(code(cand[s], cands))
        taken = jnp.sum(
            jnp.where(k_ids == choice[pl.ds(s, 1), :], coded[i], 0), axis=0, keepdims=True
        )
        wants.append(jnp.where(live & (iota((slots, halos), 0) == rank), taken, 0).astype(F32))
    blank = jnp.zeros((slots, halos), F32)
    table_of = [
        jnp.concatenate([wants[i] if i == j else blank for i in range(snaps)], axis=1) for j in range(snaps)
    ]
    table_of.append(jnp.zeros((128 - snaps * slots, snaps * halos), F32))
    told = dot_nt(
        jnp.concatenate([hot(v) for v in named], axis=1), jnp.concatenate(table_of, axis=0).astype(BF16)
    )
    send_want[...] = told.reshape(n, 1, 128)

    blocks, rows = [], []
    for ls in range(own):
        s = own * core + ls
        dest, rank, _, live = route[ls]
        listed = jnp.where(k_ids < lengths[pl.ds(s, 1), :], coded[ls], 0)
        taken = jnp.sum(jnp.where(k_ids == choice[pl.ds(s, 1), :], coded[ls], 0), axis=0, keepdims=True)
        parts = [listed, jnp.broadcast_to(taken, (GROUP - k_count, halos))]
        parts = [jnp.zeros((GROUP * ls, halos), jnp.int32)] * (ls > 0) + parts
        if ls < own - 1:
            parts.append(jnp.zeros((GROUP * (own - 1 - ls), halos), jnp.int32))
        blocks.append(jnp.concatenate(parts, axis=0).astype(F32).astype(BF16))
        rows.append(
            [
                jnp.where(live & (rank >= g * hs) & (rank < (g + 1) * hs), dest * hs + rank - g * hs, -1)
                for g in range(2)
            ]
        )
    block = jnp.concatenate(blocks, axis=1)
    blank = jnp.zeros_like(block)
    meta = sum(
        dot_nt(
            jnp.concatenate([hot(iota((n * hs, halos), 0) == r[g]) for r in rows], axis=1),
            jnp.concatenate([blank, block] if g else [block, blank], axis=0),
        )
        for g in range(2)
    )
    send_meta[...] = meta.astype(BF16).reshape(n, hs, 128)

    loads[5].wait()
    for i, (x, ls) in enumerate(order):
        place = hot(iota((total, halos), 0) == route[i][2])
        packed = dot(place, halo[own * core_of(x) + ls]).astype(BF16)
        send[x * n : (x + 1) * n, ls] = packed.reshape(n, slots, half)

    pl.semaphore_wait(barrier, 2 * n - 1)

    each_chip(
        lambda peer: remote(
            send_want.at[peer], recv_want.at[me], want_sem.at[0], want_sem.at[1], peer, 0
        ).start()
    )
    each_chip(
        lambda peer: remote(
            send_meta.at[peer], recv_meta.at[me], meta_sem.at[0], meta_sem.at[1], peer, 0
        ).start()
    )
    def row_copy(peer, x):
        return remote(
            send.at[x * n + peer], recv.at[x * n + me], row_sem.at[x], row_sem.at[2 + x], peer, x
        )

    each_chip(lambda peer: row_copy(peer, 0).start())
    each_chip(lambda peer: row_copy(peer, 1).start())
    row_copy(me, 1).start()
    table_copy = remote(
        desc_in.at[pl.ds(own * core_of(1), own)], table, table_sem.at[0], table_sem.at[1], me, 1
    )
    table_copy.start()
    recv_want[me] = send_want[me]
    recv_meta[me] = send_meta[me]
    recv[me] = send[me]

    lines = [v.astype(F32) for dest, rank, target, live in route for v in (dest, jnp.where(live, rank, -128), target)]
    lines = jnp.concatenate(lines + [jnp.zeros((128 - len(lines), halos), F32)], axis=0).T
    back = []
    lane = iota((halos, 128), 1).astype(F32)
    for i in range(snaps):
        dest, rank, target = [lines[:, 3 * i + j : 3 * i + j + 1] for j in range(3)]
        back.append(
            (
                hot(iota((halos, n), 1).astype(F32) == dest),
                (lane == rank + 3 * slots * (i % own)) | (lane == rank + (3 * (i % own) + 1) * slots),
                lane == rank + (3 * (i % own) + 2) * slots,
                hot(iota((halos, total), 1).astype(F32) == target),
            )
        )
    entry = iota((n * hs, total), 0)
    column = iota((n * hs, total), 1)
    inside = column % slots
    unpack = [
        hot((entry == (column // slots) * hs + inside - g * hs) & (inside // hs == g)) for g in range(2)
    ]
    loads[6].wait()

    ids = code(iota((total, cands), 1), cands).astype(F32)
    from_chip = hot(iota((total, n), 1) == iota((total, n), 0) // slots)
    its_slot = iota((total, 128), 1) % slots == iota((total, 128), 0) % slots
    part = [hot(iota((128, 128), 0) // slots == i) for i in range(snaps)]

    whole(recv_want.at[pl.ds(0, n - 1)], want_sem.at[0], want_sem.at[1]).wait_recv()
    wanted = dot(from_chip, recv_want[...].reshape(n, 128).astype(BF16))
    wanted = jnp.where(its_slot, wanted, 0.0).astype(BF16)
    for i, (x, ls) in enumerate(order):
        at = jnp.concatenate([dot(wanted, part[i])] * (cands // 128), axis=1)
        chosen = dot(hot(at == ids), desc[own * core_of(x) + ls]).astype(BF16)
        pick[:, 2 * ls + x] = chosen.reshape(n, slots, half)
    step = 64
    whole(recv_meta.at[pl.ds(0, n - 1)], meta_sem.at[0], meta_sem.at[1]).wait_recv()
    arrived = recv_meta[...].reshape(n * hs, 128).astype(F32).T.astype(BF16)
    picks = []
    for ls in range(own):
        lists = sum(
            dot(arrived[(g * own + ls) * GROUP : (g * own + ls + 1) * GROUP], unpack[g]) for g in range(2)
        )
        picks.append(lists[k_count : k_count + 1])

        listed = lists[:k_count].astype(jnp.int32)
        at = listed + cands // 2 - jnp.where(listed > 0, 1, 0)
        flag = jnp.where(listed == 0, 0, jnp.left_shift(1, at & 31))
        at = at >> 5
        words = jnp.zeros((cands // 32, total), jnp.int32)
        for k in range(k_count):
            words = words | jnp.where(iota((cands // 32, total), 0) == at[k : k + 1], flag[k : k + 1], 0)
        bit = jnp.left_shift(1, iota((32, total), 0))
        for w in range(cands // 32):
            bias[ls, 32 * w : 32 * w + 32, :] = jnp.where((words[w : w + 1] & bit) != 0, 0.0, NEG)

    scale = 1.0 / math.sqrt(width)
    owned = iota((n, total), 0) == iota((n, total), 1) // slots
    fold = [
        jnp.concatenate(
            [
                hot(iota((total, 128), 1) == (3 * ls + part) * slots + iota((total, 128), 0) % slots)
                for part in range(3)
            ],
            axis=0,
        )
        for ls in range(own)
    ]

    whole(recv.at[pl.ds(0, n - 1)], row_sem.at[0], row_sem.at[2]).wait_recv()
    each_chip(
        lambda peer: remote(
            pick.at[peer], recv_pick.at[me], pick_sem.at[0], pick_sem.at[1], peer, 0
        ).start()
    )
    recv_pick[me] = pick[me]

    told = None
    table_copy.wait_recv()
    whole(recv.at[pl.ds(n, n)], row_sem.at[1], row_sem.at[3]).wait_recv()
    for ls in range(own):
        scores[ls] = dot_nt(
            jnp.concatenate([desc[own * core + ls], table[ls]], axis=1),
            jnp.concatenate(
                [recv[x * n : (x + 1) * n, ls].reshape(total, half) for x in range(2)], axis=1
            ),
        )

        def chunk(i, carry):
            top, picked, claimed = carry
            at = pl.ds(pl.multiple_of(i * step, step), step)
            value = scores[ls, at, :]
            masked = value + bias[ls, at, :]
            claim = jnp.max(masked, axis=1, keepdims=True)
            chosen = code(iota((step, total), 0) + i * step, cands).astype(F32) == picks[ls]

            def least(v):
                return jnp.max(v.reshape(step // 8, 8, total), axis=0)

            return (
                jnp.maximum(top, least(masked)),
                jnp.maximum(picked, least(jnp.where(chosen, value, NEG))),
                jnp.maximum(claimed, least(jnp.where(chosen, claim, NEG))),
            )

        start = jnp.full((8, total), NEG, F32)
        top, picked, claimed = [
            jnp.max(v, axis=0, keepdims=True)
            for v in lax.fori_loop(0, cands // step, chunk, (start, start, start), unroll=True)
        ]

        def quality(v):
            v = v * scale
            return 1.0 + jnp.maximum(v, 0.0) + jnp.log(1.0 + jnp.exp(-jnp.abs(v)))

        mine = quality(picked)
        share = mine / (mine + quality(claimed))
        high = share.astype(BF16).astype(F32)
        top = jnp.where(top > NEG * 0.5, top * scale, 0.0)
        spread = jnp.concatenate(
            [jnp.where(owned, jnp.broadcast_to(v, (n, total)), 0.0) for v in (high, share - high, top)],
            axis=1,
        ).astype(BF16)
        term = dot(spread, fold[ls])
        told = term if told is None else told + term
    res[...] = told.reshape(n, 1, 128)
    each_peer(
        lambda peer, x: remote(
            res.at[peer], recv_res.at[x * n + me], res_sem.at[0], res_sem.at[1], peer, x
        ).start()
    )
    recv_res[me] = res[me]

    ones = jnp.ones((128, half), BF16)
    tops = []
    whole(recv_pick.at[pl.ds(0, n - 1)], pick_sem.at[0], pick_sem.at[1]).wait_recv()
    rows = [
        dot(back[x * own + ls][3], recv_pick[:, 2 * ls + x].reshape(total, half)) for x, ls in order
    ]
    whole(recv_res.at[pl.ds(0, 2 * n - 1)], res_sem.at[0], res_sem.at[1]).wait_recv()
    for i, (x, ls) in enumerate(order):
        s = own * core_of(x) + ls
        named, shared, topped, _ = back[i]
        brought = recv_res[x * n : (x + 1) * n].reshape(n, 128).astype(BF16)
        spread = dot(named, brought)
        share = dot(jnp.where(shared, spread, 0.0).astype(BF16), ones)
        phantom[s] = ((1.0 - share) * halo[s].astype(F32) + share * rows[i]).astype(BF16)
        tops.append(dot_nt(ones[0:8], jnp.where(topped, spread, 0.0).astype(BF16))[0:1])
    first, second = jnp.concatenate(tops[:own], axis=0), jnp.concatenate(tops[own:], axis=0)
    even = core == 0
    best[...] = jnp.concatenate(
        [jnp.where(even, first, second), jnp.where(even, second, first)], axis=0
    ).astype(BF16)

    table_copy.wait_send()
    whole(send_want.at[pl.ds(0, n - 1)], want_sem.at[0], want_sem.at[1]).wait_send()
    whole(send_meta.at[pl.ds(0, n - 1)], meta_sem.at[0], meta_sem.at[1]).wait_send()
    whole(send.at[pl.ds(0, n - 1)], row_sem.at[0], row_sem.at[2]).wait_send()
    whole(send.at[pl.ds(0, n)], row_sem.at[1], row_sem.at[3]).wait_send()
    whole(pick.at[pl.ds(0, n - 1)], pick_sem.at[0], pick_sem.at[1]).wait_send()
    whole(recv_res.at[pl.ds(0, 2 * n - 1)], res_sem.at[0], res_sem.at[1]).wait_send()


def hand_over(phantom_in, best_in, phantom, best):
    phantom[...] = phantom_in[...]
    best[...] = best_in[...]


def body(n, halo_rows, unmatched, owner_id, cand_index, lengths, choice_index, desc_rows):
    snaps, halos, half = halo_rows.shape
    cands = desc_rows.shape[1]
    own = snaps // 2
    slots = max(2 * halos // n, 16)
    total = n * slots
    dma = pltpu.SemaphoreType.DMA
    results = pl.pallas_call(
        functools.partial(kernel, n, slots, 2 * half),
        out_shape=(
            pltpu.VMEM((snaps, halos, half), BF16),
            pltpu.VMEM((snaps, halos), BF16),
        ),
        in_specs=[pl.BlockSpec(memory_space=pl.ANY)] * 7,
        out_specs=(pl.BlockSpec(memory_space=pltpu.VMEM),) * 2,
        scratch_shapes=[
            pltpu.VMEM(halo_rows.shape, BF16),
            pltpu.VMEM(unmatched.shape, jnp.int32),
            pltpu.VMEM((snaps, 1, halos), jnp.int32),
            pltpu.VMEM((snaps, cand_index.shape[2], halos), jnp.int32),
            pltpu.VMEM(lengths.shape, jnp.int32),
            pltpu.VMEM(choice_index.shape, jnp.int32),
            pltpu.VMEM((snaps, cands, half), BF16),
            pltpu.VMEM((own, cands, half), BF16),
            pltpu.VMEM((2 * n, own, slots, half), BF16),
            pltpu.VMEM((2 * n, own, slots, half), BF16),
            pltpu.VMEM((n, 1, 128), F32),
            pltpu.VMEM((n, 1, 128), F32),
            pltpu.VMEM((n, slots // 2, 128), BF16),
            pltpu.VMEM((n, slots // 2, 128), BF16),
            pltpu.VMEM((own, cands, total), F32),
            pltpu.VMEM((own, cands, total), F32),
            pltpu.VMEM((n, snaps, slots, half), BF16),
            pltpu.VMEM((n, snaps, slots, half), BF16),
            pltpu.VMEM((n, 1, 128), F32),
            pltpu.VMEM((2 * n, 1, 128), F32),
            dma((4,)), dma((2,)), dma((2,)), dma((2,)), dma((2,)), dma((2,)), dma((7,)),
        ],
        compiler_params=pltpu.CompilerParams(collective_id=0, has_side_effects=True),
    )(
        halo_rows,
        unmatched,
        jnp.swapaxes(owner_id, 1, 2),
        jnp.swapaxes(cand_index, 1, 2),
        lengths,
        choice_index,
        desc_rows,
    )
    shapes = tuple(jax.ShapeDtypeStruct(v.shape, v.dtype) for v in results)
    return pl.pallas_call(
        hand_over,
        out_shape=shapes,
        in_specs=[pl.BlockSpec(memory_space=pltpu.VMEM)] * 2,
        out_specs=(pl.BlockSpec(memory_space=pltpu.VMEM),) * 2,
    )(*[pltpu.with_memory_space_constraint(v, pltpu.VMEM) for v in results])


def solution(mesh):
    in_specs = (
        P(None, "space", "rep"),
        P(None, "space"),
        P(None, "space", None),
        P(None, "space", None),
        P(None, "space"),
        P(None, "space"),
        P(None, "space", "rep"),
    )
    out_specs = (P(None, "space", "rep"), P(None, "space"))
    return jax.shard_map(
        functools.partial(body, mesh.shape["space"]),
        mesh=mesh, in_specs=in_specs, out_specs=out_specs, check_vma=False,
    )
```

```python
import functools
import math

import jax
import jax.numpy as jnp
from jax import lax
from jax.experimental import pallas as pl
from jax.experimental.pallas import tpu as pltpu
from jax.sharding import PartitionSpec as P

MESH = pl.DeviceIdType.MESH
F32 = jnp.float32
BF16 = jnp.bfloat16
NEG = -1e30
GROUP = 32
NT = (((1,), (1,)), ((), ()))


def iota(shape, dim):
    return lax.broadcasted_iota(jnp.int32, shape, dim)


def dot(a, b):
    return jnp.dot(a, b, preferred_element_type=F32)


def dot_nt(a, b):
    return lax.dot_general(a, b, NT, preferred_element_type=F32)


def hot(mask):
    return jnp.where(mask, 1.0, 0.0).astype(BF16)


def code(index, cands):
    return index - cands // 2 + jnp.where(index >= cands // 2, 1, 0)


def kernel(
    n, slots, width,
    halo_in, unmatched_in, owner_in, cand_in, lengths_in, choice_in, desc_in,
    phantom, best,
    halo, unmatched, owner, cand, lengths, choice, desc, table,
    send, recv, send_want, recv_want, send_meta, recv_meta, scores, bias, pick, recv_pick, res, recv_res,
    row_sem, want_sem, meta_sem, pick_sem, res_sem, table_sem, load_sem,
):
    me, core = lax.axis_index("space"), lax.axis_index("rep")
    snaps, halos, half = halo.shape
    k_count = cand.shape[1]
    cands = desc.shape[1]
    own = snaps // 2
    total = n * slots
    hs = slots // 2

    def core_of(x):
        return 1 - core if x else core

    def remote(src, dst, ss, rs, peer, x):
        return pltpu.make_async_remote_copy(
            src_ref=src, dst_ref=dst, send_sem=ss, recv_sem=rs,
            device_id=(peer, core_of(x)), device_id_type=MESH,
        )

    def whole(ref, ss, rs):
        return remote(ref, ref, ss, rs, me, 1)

    def each_chip(f, part=None):
        if n % 4 or n > 32:
            low, high = {None: (1, n), 0: (1, n // 2), 1: (n // 2, n)}[part]

            @pl.loop(low, high)
            def _(d):
                peer = me + d
                f(jnp.where(peer >= n, peer - n, peer))

            return
        blocks = [*range(1, n // 4), 0]
        if part is not None:
            blocks = blocks[n // 8 :] if part else blocks[: n // 8]
        block, place = me // 4, lax.rem(me, 4)
        for d in blocks:
            to = block + d
            to = jnp.where(to >= n // 4, to - n // 4, to) * 4
            for q in (3, 1, 2, 0):
                if d or q:
                    f(to + jnp.bitwise_xor(place, q))

    def each_peer(f):
        def both(peer):
            f(peer, 0)
            f(peer, 1)

        each_chip(both)
        f(me, 1)

    barrier = pltpu.get_barrier_semaphore()
    each_peer(
        lambda peer, x: pl.semaphore_signal(
            barrier, inc=1, device_id=(peer, core_of(x)), device_id_type=MESH
        ),
    )
    loads = [
        pltpu.make_async_copy(src, dst, load_sem.at[i])
        for i, (src, dst) in enumerate(
            [
                (owner_in, owner), (unmatched_in, unmatched), (cand_in, cand),
                (lengths_in, lengths), (choice_in, choice), (halo_in, halo), (desc_in, desc),
            ]
        )
    ]
    for load in loads:
        load.start()
    for load in loads[:5]:
        load.wait()

    order = [(x, ls) for x in range(2) for ls in range(own)]
    named = [iota((n, halos), 0) == owner[own * core_of(x) + ls] for x, ls in order]
    onehot = hot(jnp.concatenate(named, axis=0))
    before = dot(onehot, hot(iota((halos, halos), 0) < iota((halos, halos), 1)))
    route = []
    for i, (x, ls) in enumerate(order):
        s = own * core_of(x) + ls
        rank = jnp.sum(
            jnp.where(named[i], before[i * n : (i + 1) * n], 0.0), axis=0, keepdims=True
        ).astype(jnp.int32)
        live = unmatched[pl.ds(s, 1), :] == 1
        dest = owner[s]
        route.append((dest, rank, jnp.where(live, dest * slots + rank, -1), live))

    k_ids = iota((k_count, halos), 0)
    wants, coded = [], []
    for i, (x, ls) in enumerate(order):
        s = own * core_of(x) + ls
        _, rank, _, live = route[i]
        coded.append(code(cand[s], cands))
        taken = jnp.sum(
            jnp.where(k_ids == choice[pl.ds(s, 1), :], coded[i], 0), axis=0, keepdims=True
        )
        wants.append(jnp.where(live & (iota((slots, halos), 0) == rank), taken, 0).astype(F32))
    blank = jnp.zeros((slots, halos), F32)
    table_of = [
        jnp.concatenate([wants[i] if i == j else blank for i in range(snaps)], axis=1) for j in range(snaps)
    ]
    table_of.append(jnp.zeros((128 - snaps * slots, snaps * halos), F32))
    told = dot_nt(
        jnp.concatenate([hot(v) for v in named], axis=1), jnp.concatenate(table_of, axis=0).astype(BF16)
    )
    send_want[...] = told.reshape(n, 1, 128)

    blocks, rows = [], []
    for ls in range(own):
        s = own * core + ls
        dest, rank, _, live = route[ls]
        listed = jnp.where(k_ids < lengths[pl.ds(s, 1), :], coded[ls], 0)
        taken = jnp.sum(jnp.where(k_ids == choice[pl.ds(s, 1), :], coded[ls], 0), axis=0, keepdims=True)
        parts = [listed, jnp.broadcast_to(taken, (GROUP - k_count, halos))]
        parts = [jnp.zeros((GROUP * ls, halos), jnp.int32)] * (ls > 0) + parts
        if ls < own - 1:
            parts.append(jnp.zeros((GROUP * (own - 1 - ls), halos), jnp.int32))
        blocks.append(jnp.concatenate(parts, axis=0).astype(F32).astype(BF16))
        rows.append(
            [
                jnp.where(live & (rank >= g * hs) & (rank < (g + 1) * hs), dest * hs + rank - g * hs, -1)
                for g in range(2)
            ]
        )
    block = jnp.concatenate(blocks, axis=1)
    blank = jnp.zeros_like(block)
    meta = sum(
        dot_nt(
            jnp.concatenate([hot(iota((n * hs, halos), 0) == r[g]) for r in rows], axis=1),
            jnp.concatenate([blank, block] if g else [block, blank], axis=0),
        )
        for g in range(2)
    )
    send_meta[...] = meta.astype(BF16).reshape(n, hs, 128)

    loads[5].wait()
    for i, (x, ls) in enumerate(order):
        place = hot(iota((total, halos), 0) == route[i][2])
        packed = dot(place, halo[own * core_of(x) + ls]).astype(BF16)
        send[x * n : (x + 1) * n, ls] = packed.reshape(n, slots, half)

    pl.semaphore_wait(barrier, 2 * n - 1)

    each_chip(
        lambda peer: remote(
            send_want.at[peer], recv_want.at[me], want_sem.at[0], want_sem.at[1], peer, 0
        ).start()
    )
    each_chip(
        lambda peer: remote(
            send_meta.at[peer], recv_meta.at[me], meta_sem.at[0], meta_sem.at[1], peer, 0
        ).start()
    )
    def row_copy(peer, x):
        return remote(
            send.at[x * n + peer], recv.at[x * n + me], row_sem.at[x], row_sem.at[2 + x], peer, x
        )

    each_chip(lambda peer: row_copy(peer, 0).start())
    each_chip(lambda peer: row_copy(peer, 1).start())
    row_copy(me, 1).start()
    table_copy = remote(
        desc_in.at[pl.ds(own * core_of(1), own)], table, table_sem.at[0], table_sem.at[1], me, 1
    )
    table_copy.start()
    recv_want[me] = send_want[me]
    recv_meta[me] = send_meta[me]
    recv[me] = send[me]

    lines = [v.astype(F32) for dest, rank, target, live in route for v in (dest, jnp.where(live, rank, -128), target)]
    lines = jnp.concatenate(lines + [jnp.zeros((128 - len(lines), halos), F32)], axis=0).T
    back = []
    lane = iota((halos, 128), 1).astype(F32)
    for i in range(snaps):
        dest, rank, target = [lines[:, 3 * i + j : 3 * i + j + 1] for j in range(3)]
        back.append(
            (
                hot(iota((halos, n), 1).astype(F32) == dest),
                functools.reduce(
                    jnp.logical_or, [lane == rank + (3 * (i % own) + part) * slots for part in range(3)]
                ),
                hot(iota((halos, total), 1).astype(F32) == target),
            )
        )
    entry = iota((n * hs, total), 0)
    column = iota((n * hs, total), 1)
    inside = column % slots
    unpack = [
        hot((entry == (column // slots) * hs + inside - g * hs) & (inside // hs == g)) for g in range(2)
    ]
    loads[6].wait()

    ids = code(iota((total, cands), 1), cands).astype(F32)
    from_chip = hot(iota((total, n), 1) == iota((total, n), 0) // slots)
    its_slot = iota((total, 128), 1) % slots == iota((total, 128), 0) % slots
    part = [hot(iota((128, 128), 0) // slots == i) for i in range(snaps)]

    whole(recv_want.at[pl.ds(0, n - 1)], want_sem.at[0], want_sem.at[1]).wait_recv()
    wanted = dot(from_chip, recv_want[...].reshape(n, 128).astype(BF16))
    wanted = jnp.where(its_slot, wanted, 0.0).astype(BF16)
    for i, (x, ls) in enumerate(order):
        at = jnp.concatenate([dot(wanted, part[i])] * (cands // 128), axis=1)
        chosen = dot(hot(at == ids), desc[own * core_of(x) + ls]).astype(BF16)
        pick[:, 2 * ls + x] = chosen.reshape(n, slots, half)
    step = 64
    whole(recv_meta.at[pl.ds(0, n - 1)], meta_sem.at[0], meta_sem.at[1]).wait_recv()
    arrived = recv_meta[...].reshape(n * hs, 128).astype(F32).T.astype(BF16)
    picks = []
    for ls in range(own):
        lists = sum(
            dot(arrived[(g * own + ls) * GROUP : (g * own + ls + 1) * GROUP], unpack[g]) for g in range(2)
        )
        picks.append(lists[k_count : k_count + 1])

        listed = lists[:k_count].astype(jnp.int32)
        at = listed + cands // 2 - jnp.where(listed > 0, 1, 0)
        flag = jnp.where(listed == 0, 0, jnp.left_shift(1, at & 31))
        at = at >> 5
        words = jnp.zeros((cands // 32, total), jnp.int32)
        for k in range(k_count):
            words = words | jnp.where(iota((cands // 32, total), 0) == at[k : k + 1], flag[k : k + 1], 0)
        bit = jnp.left_shift(1, iota((32, total), 0))
        for w in range(cands // 32):
            bias[ls, 32 * w : 32 * w + 32, :] = jnp.where((words[w : w + 1] & bit) != 0, 0.0, NEG)

    scale = 1.0 / math.sqrt(width)
    owned = iota((n, total), 0) == iota((n, total), 1) // slots
    fold = [
        jnp.concatenate(
            [
                hot(iota((total, 128), 1) == (3 * ls + part) * slots + iota((total, 128), 0) % slots)
                for part in range(3)
            ],
            axis=0,
        )
        for ls in range(own)
    ]

    whole(recv.at[pl.ds(0, n - 1)], row_sem.at[0], row_sem.at[2]).wait_recv()
    def pick_copy(peer):
        return remote(
            pick.at[peer], recv_pick.at[me], pick_sem.at[0], pick_sem.at[1], peer, 0
        )

    each_chip(lambda peer: pick_copy(peer).start(), 0)
    recv_pick[me] = pick[me]

    told = None
    table_copy.wait_recv()
    whole(recv.at[pl.ds(n, n)], row_sem.at[1], row_sem.at[3]).wait_recv()
    for ls in range(own):
        scores[ls] = dot_nt(
            jnp.concatenate([desc[own * core + ls], table[ls]], axis=1),
            jnp.concatenate(
                [recv[x * n : (x + 1) * n, ls].reshape(total, half) for x in range(2)], axis=1
            ),
        )

        def chunk(i, carry):
            top, picked, claimed = carry
            at = pl.ds(pl.multiple_of(i * step, step), step)
            value = scores[ls, at, :]
            masked = value + bias[ls, at, :]
            claim = jnp.max(masked, axis=1, keepdims=True)
            chosen = code(iota((step, total), 0) + i * step, cands).astype(F32) == picks[ls]

            def least(v):
                return jnp.max(v.reshape(step // 8, 8, total), axis=0)

            return (
                jnp.maximum(top, least(masked)),
                jnp.maximum(picked, least(jnp.where(chosen, value, NEG))),
                jnp.maximum(claimed, least(jnp.where(chosen, claim, NEG))),
            )

        start = jnp.full((8, total), NEG, F32)
        top, picked, claimed = [
            jnp.max(v, axis=0, keepdims=True)
            for v in lax.fori_loop(0, cands // step, chunk, (start, start, start), unroll=True)
        ]

        def quality(v):
            v = v * scale
            return 1.0 + jnp.maximum(v, 0.0) + jnp.log(1.0 + jnp.exp(-jnp.abs(v)))

        mine = quality(picked)
        share = mine / (mine + quality(claimed))
        high = share.astype(BF16).astype(F32)
        top = jnp.where(top > NEG * 0.5, top * scale, 0.0)
        spread = jnp.concatenate(
            [jnp.where(owned, jnp.broadcast_to(v, (n, total)), 0.0) for v in (high, share - high, top)],
            axis=1,
        ).astype(BF16)
        term = dot(spread, fold[ls])
        told = term if told is None else told + term
    res[...] = told.reshape(n, 1, 128)
    each_peer(
        lambda peer, x: remote(
            res.at[peer], recv_res.at[x * n + me], res_sem.at[0], res_sem.at[1], peer, x
        ).start()
    )
    recv_res[me] = res[me]
    each_chip(lambda peer: pick_copy(peer).start(), 1)

    kind = iota((128, half + halos), 0) // slots % 3
    first = iota((128, half + halos), 1) < half
    merge = hot((first & (kind < 2)) | (~first & (kind == 2)))
    eye = iota((halos, halos), 0) == iota((halos, halos), 1)
    whole(recv_pick.at[pl.ds(0, n - 1)], pick_sem.at[0], pick_sem.at[1]).wait_recv()
    rows = [
        dot(back[i][2], recv_pick[:, 2 * ls + x].reshape(total, half)) for i, (x, ls) in enumerate(order)
    ]
    whole(recv_res.at[pl.ds(0, 2 * n - 1)], res_sem.at[0], res_sem.at[1]).wait_recv()
    spread = [
        dot(
            jnp.concatenate([back[x * own + ls][0] for ls in range(own)], axis=0),
            recv_res[x * n : (x + 1) * n].reshape(n, 128).astype(BF16),
        )
        for x in range(2)
    ]
    spread = jnp.where(
        jnp.concatenate([v[1] for v in back], axis=0), jnp.concatenate(spread, axis=0), 0.0
    ).astype(BF16)
    spread = dot(spread, merge)
    tops = []
    for i, (x, ls) in enumerate(order):
        s = own * core_of(x) + ls
        share = spread[i * halos : (i + 1) * halos, :half]
        phantom[s] = ((1.0 - share) * halo[s].astype(F32) + share * rows[i]).astype(BF16)
        tops.append(
            jnp.sum(jnp.where(eye, spread[i * halos : (i + 1) * halos, half:], 0.0), axis=0, keepdims=True)
        )
    first, second = jnp.concatenate(tops[:own], axis=0), jnp.concatenate(tops[own:], axis=0)
    even = core == 0
    best[...] = jnp.concatenate(
        [jnp.where(even, first, second), jnp.where(even, second, first)], axis=0
    ).astype(BF16)

    table_copy.wait_send()
    whole(send_want.at[pl.ds(0, n - 1)], want_sem.at[0], want_sem.at[1]).wait_send()
    whole(send_meta.at[pl.ds(0, n - 1)], meta_sem.at[0], meta_sem.at[1]).wait_send()
    whole(send.at[pl.ds(0, n - 1)], row_sem.at[0], row_sem.at[2]).wait_send()
    whole(send.at[pl.ds(0, n)], row_sem.at[1], row_sem.at[3]).wait_send()
    whole(pick.at[pl.ds(0, n - 1)], pick_sem.at[0], pick_sem.at[1]).wait_send()
    whole(recv_res.at[pl.ds(0, 2 * n - 1)], res_sem.at[0], res_sem.at[1]).wait_send()


def hand_over(phantom_in, best_in, phantom, best):
    phantom[...] = phantom_in[...]
    best[...] = best_in[...]


def body(n, halo_rows, unmatched, owner_id, cand_index, lengths, choice_index, desc_rows):
    snaps, halos, half = halo_rows.shape
    cands = desc_rows.shape[1]
    own = snaps // 2
    slots = max(2 * halos // n, 16)
    total = n * slots
    dma = pltpu.SemaphoreType.DMA
    results = pl.pallas_call(
        functools.partial(kernel, n, slots, 2 * half),
        out_shape=(
            pltpu.VMEM((snaps, halos, half), BF16),
            pltpu.VMEM((snaps, halos), BF16),
        ),
        in_specs=[pl.BlockSpec(memory_space=pl.ANY)] * 7,
        out_specs=(pl.BlockSpec(memory_space=pltpu.VMEM),) * 2,
        scratch_shapes=[
            pltpu.VMEM(halo_rows.shape, BF16),
            pltpu.VMEM(unmatched.shape, jnp.int32),
            pltpu.VMEM((snaps, 1, halos), jnp.int32),
            pltpu.VMEM((snaps, cand_index.shape[2], halos), jnp.int32),
            pltpu.VMEM(lengths.shape, jnp.int32),
            pltpu.VMEM(choice_index.shape, jnp.int32),
            pltpu.VMEM((snaps, cands, half), BF16),
            pltpu.VMEM((own, cands, half), BF16),
            pltpu.VMEM((2 * n, own, slots, half), BF16),
            pltpu.VMEM((2 * n, own, slots, half), BF16),
            pltpu.VMEM((n, 1, 128), F32),
            pltpu.VMEM((n, 1, 128), F32),
            pltpu.VMEM((n, slots // 2, 128), BF16),
            pltpu.VMEM((n, slots // 2, 128), BF16),
            pltpu.VMEM((own, cands, total), F32),
            pltpu.VMEM((own, cands, total), F32),
            pltpu.VMEM((n, snaps, slots, half), BF16),
            pltpu.VMEM((n, snaps, slots, half), BF16),
            pltpu.VMEM((n, 1, 128), F32),
            pltpu.VMEM((2 * n, 1, 128), F32),
            dma((4,)), dma((2,)), dma((2,)), dma((2,)), dma((2,)), dma((2,)), dma((7,)),
        ],
        compiler_params=pltpu.CompilerParams(collective_id=0, has_side_effects=True),
    )(
        halo_rows,
        unmatched,
        jnp.swapaxes(owner_id, 1, 2),
        jnp.swapaxes(cand_index, 1, 2),
        lengths,
        choice_index,
        desc_rows,
    )
    shapes = tuple(jax.ShapeDtypeStruct(v.shape, v.dtype) for v in results)
    return pl.pallas_call(
        hand_over,
        out_shape=shapes,
        in_specs=[pl.BlockSpec(memory_space=pltpu.VMEM)] * 2,
        out_specs=(pl.BlockSpec(memory_space=pltpu.VMEM),) * 2,
    )(*[pltpu.with_memory_space_constraint(v, pltpu.VMEM) for v in results])


def solution(mesh):
    in_specs = (
        P(None, "space", "rep"),
        P(None, "space"),
        P(None, "space", None),
        P(None, "space", None),
        P(None, "space"),
        P(None, "space"),
        P(None, "space", "rep"),
    )
    out_specs = (P(None, "space", "rep"), P(None, "space"))
    return jax.shard_map(
        functools.partial(body, mesh.shape["space"]),
        mesh=mesh, in_specs=in_specs, out_specs=out_specs, check_vma=False,
    )
```

```python
import functools
import math

import jax
import jax.numpy as jnp
from jax import lax
from jax.experimental import pallas as pl
from jax.experimental.pallas import tpu as pltpu
from jax.sharding import PartitionSpec as P

MESH = pl.DeviceIdType.MESH
F32 = jnp.float32
BF16 = jnp.bfloat16
NEG = -1e30
PARTS = 4
NT = (((1,), (1,)), ((), ()))


def iota(shape, dim):
    return lax.broadcasted_iota(jnp.int32, shape, dim)


def dot(a, b):
    return jnp.dot(a, b, preferred_element_type=F32)


def dot_nt(a, b):
    return lax.dot_general(a, b, NT, preferred_element_type=F32)


def hot(mask):
    return jnp.where(mask, 1.0, 0.0).astype(BF16)


def code(index, cands):
    return index - cands // 2 + jnp.where(index >= cands // 2, 1, 0)


def kernel(
    n, slots, width,
    halo_in, unmatched_in, owner_in, cand_in, lengths_in, choice_in, desc_in,
    phantom, best,
    halo, unmatched, owner, cand, lengths, choice, desc, table,
    send, recv, send_want, recv_want, send_meta, recv_meta, scores, bias, pick, recv_pick, res, recv_res,
    row_sem, want_sem, meta_sem, pick_sem, res_sem, table_sem, load_sem,
):
    me, core = lax.axis_index("space"), lax.axis_index("rep")
    snaps, halos, half = halo.shape
    k_count = cand.shape[1]
    cands = desc.shape[1]
    own = snaps // 2
    total = n * slots
    qs = slots // PARTS

    def core_of(x):
        return 1 - core if x else core

    def remote(src, dst, ss, rs, peer, x):
        return pltpu.make_async_remote_copy(
            src_ref=src, dst_ref=dst, send_sem=ss, recv_sem=rs,
            device_id=(peer, core_of(x)), device_id_type=MESH,
        )

    def whole(ref, ss, rs):
        return remote(ref, ref, ss, rs, me, 1)

    def each_chip(f, part=None):
        if n % 4 or n > 32:
            low, high = {None: (1, n), 0: (1, n // 2), 1: (n // 2, n)}[part]

            @pl.loop(low, high)
            def _(d):
                peer = me + d
                f(jnp.where(peer >= n, peer - n, peer))

            return
        blocks = [*range(1, n // 4), 0]
        if part is not None:
            blocks = blocks[n // 8 :] if part else blocks[: n // 8]
        block, place = me // 4, lax.rem(me, 4)
        for d in blocks:
            to = block + d
            to = jnp.where(to >= n // 4, to - n // 4, to) * 4
            for q in (3, 1, 2, 0):
                if d or q:
                    f(to + jnp.bitwise_xor(place, q))

    def each_peer(f):
        def both(peer):
            f(peer, 0)
            f(peer, 1)

        each_chip(both)
        f(me, 1)

    barrier = pltpu.get_barrier_semaphore()
    each_peer(
        lambda peer, x: pl.semaphore_signal(
            barrier, inc=1, device_id=(peer, core_of(x)), device_id_type=MESH
        ),
    )
    loads = [
        pltpu.make_async_copy(src, dst, load_sem.at[i])
        for i, (src, dst) in enumerate(
            [
                (owner_in, owner), (unmatched_in, unmatched), (cand_in, cand),
                (lengths_in, lengths), (choice_in, choice), (halo_in, halo), (desc_in, desc),
            ]
        )
    ]
    for load in loads:
        load.start()
    for load in loads[:5]:
        load.wait()

    order = [(x, ls) for x in range(2) for ls in range(own)]
    named = [iota((n, halos), 0) == owner[own * core_of(x) + ls] for x, ls in order]
    onehot = hot(jnp.concatenate(named, axis=0))
    before = dot(onehot, hot(iota((halos, halos), 0) < iota((halos, halos), 1)))
    route = []
    for i, (x, ls) in enumerate(order):
        s = own * core_of(x) + ls
        rank = jnp.sum(
            jnp.where(named[i], before[i * n : (i + 1) * n], 0.0), axis=0, keepdims=True
        ).astype(jnp.int32)
        live = unmatched[pl.ds(s, 1), :] == 1
        dest = owner[s]
        route.append((dest, rank, jnp.where(live, dest * slots + rank, -1), live))

    k_ids = iota((k_count, halos), 0)
    wants, coded = [], []
    for i, (x, ls) in enumerate(order):
        s = own * core_of(x) + ls
        _, rank, _, live = route[i]
        coded.append(code(cand[s], cands))
        taken = jnp.sum(
            jnp.where(k_ids == choice[pl.ds(s, 1), :], coded[i], 0), axis=0, keepdims=True
        )
        wants.append(jnp.where(live & (iota((slots, halos), 0) == rank), taken, 0).astype(F32))
    blank = jnp.zeros((slots, halos), F32)
    table_of = [
        jnp.concatenate([wants[i] if i == j else blank for i in range(snaps)], axis=1) for j in range(snaps)
    ]
    table_of.append(jnp.zeros((128 - snaps * slots, snaps * halos), F32))
    told = dot_nt(
        jnp.concatenate([hot(v) for v in named], axis=1), jnp.concatenate(table_of, axis=0).astype(BF16)
    )
    send_want[...] = told.reshape(n, 1, 128)

    blocks, rows = [], []
    for ls in range(own):
        dest, rank, _, live = route[ls]
        listed = jnp.where(k_ids < lengths[pl.ds(own * core + ls, 1), :], coded[ls], 0).astype(F32)
        none = jnp.zeros((k_count, halos), F32)
        blocks.append(jnp.concatenate([listed if i == ls else none for i in range(own)], axis=0))
        rows.append(
            [
                jnp.where(live & (rank >= g * qs) & (rank < (g + 1) * qs), dest * qs + rank - g * qs, -1)
                for g in range(PARTS)
            ]
        )
    block = jnp.concatenate(blocks, axis=1).astype(BF16)
    blank = jnp.zeros_like(block)
    meta = sum(
        dot_nt(
            jnp.concatenate([hot(iota((n * qs, halos), 0) == r[g]) for r in rows], axis=1),
            jnp.concatenate([block if i == g else blank for i in range(PARTS)], axis=0),
        )
        for g in range(PARTS)
    )
    send_meta[...] = meta.astype(BF16).reshape(n, qs, 128)

    loads[5].wait()
    for i, (x, ls) in enumerate(order):
        place = hot(iota((total, halos), 0) == route[i][2])
        packed = dot(place, halo[own * core_of(x) + ls]).astype(BF16)
        send[x * n : (x + 1) * n, ls] = packed.reshape(n, slots, half)

    pl.semaphore_wait(barrier, 2 * n - 1)

    each_chip(
        lambda peer: remote(
            send_want.at[peer], recv_want.at[me], want_sem.at[0], want_sem.at[1], peer, 0
        ).start()
    )
    each_chip(
        lambda peer: remote(
            send_meta.at[peer], recv_meta.at[me], meta_sem.at[0], meta_sem.at[1], peer, 0
        ).start()
    )
    def row_copy(peer, x):
        return remote(
            send.at[x * n + peer], recv.at[x * n + me], row_sem.at[x], row_sem.at[2 + x], peer, x
        )

    each_chip(lambda peer: row_copy(peer, 0).start())
    each_chip(lambda peer: row_copy(peer, 1).start())
    row_copy(me, 1).start()
    table_copy = remote(
        desc_in.at[pl.ds(own * core_of(1), own)], table, table_sem.at[0], table_sem.at[1], me, 1
    )
    table_copy.start()
    recv_want[me] = send_want[me]
    recv_meta[me] = send_meta[me]
    recv[me] = send[me]

    lines = [v.astype(F32) for dest, rank, target, live in route for v in (dest, jnp.where(live, rank, -128), target)]
    lines = jnp.concatenate(lines + [jnp.zeros((128 - len(lines), halos), F32)], axis=0).T
    back = []
    lane = iota((halos, 128), 1).astype(F32)
    for i in range(snaps):
        dest, rank, target = [lines[:, 3 * i + j : 3 * i + j + 1] for j in range(3)]
        back.append(
            (
                hot(iota((halos, n), 1).astype(F32) == dest),
                functools.reduce(
                    jnp.logical_or, [lane == rank + (3 * (i % own) + part) * slots for part in range(3)]
                ),
                hot(iota((halos, total), 1).astype(F32) == target),
            )
        )
    entry = iota((n * qs, total), 0)
    column = iota((n * qs, total), 1)
    inside = column % slots
    unpack = [
        hot((entry == (column // slots) * qs + inside - g * qs) & (inside // qs == g)) for g in range(PARTS)
    ]
    loads[6].wait()

    ids = code(iota((total, cands), 1), cands).astype(F32)
    from_chip = hot(iota((total, n), 1) == iota((total, n), 0) // slots)
    its_slot = iota((total, 128), 1) % slots == iota((total, 128), 0) % slots
    part = [hot(iota((128, 128), 0) // slots == i) for i in range(snaps)]

    whole(recv_want.at[pl.ds(0, n - 1)], want_sem.at[0], want_sem.at[1]).wait_recv()
    wanted = dot(from_chip, recv_want[...].reshape(n, 128).astype(BF16))
    wanted = jnp.where(its_slot, wanted, 0.0).astype(BF16)
    picks = dot_nt(hot(iota((8, 128), 1) // slots == iota((8, 128), 0)), wanted)
    for i, (x, ls) in enumerate(order):
        at = jnp.concatenate([dot(wanted, part[i])] * (cands // 128), axis=1)
        chosen = dot(hot(at == ids), desc[own * core_of(x) + ls]).astype(BF16)
        pick[:, 2 * ls + x] = chosen.reshape(n, slots, half)
    step = 64
    whole(recv_meta.at[pl.ds(0, n - 1)], meta_sem.at[0], meta_sem.at[1]).wait_recv()
    arrived = recv_meta[...].reshape(n * qs, 128).astype(F32).T.astype(BF16)
    for ls in range(own):
        lists = sum(
            dot(arrived[(g * own + ls) * k_count : (g * own + ls + 1) * k_count], unpack[g])
            for g in range(PARTS)
        )
        listed = lists.astype(jnp.int32)
        at = listed + cands // 2 - jnp.where(listed > 0, 1, 0)
        flag = jnp.where(listed == 0, 0, jnp.left_shift(1, at & 31))
        at = at >> 5
        words = jnp.zeros((cands // 32, total), jnp.int32)
        for k in range(k_count):
            words = words | jnp.where(iota((cands // 32, total), 0) == at[k : k + 1], flag[k : k + 1], 0)
        bit = jnp.left_shift(1, iota((32, total), 0))
        for w in range(cands // 32):
            bias[ls, 32 * w : 32 * w + 32, :] = jnp.where((words[w : w + 1] & bit) != 0, 0.0, NEG)

    scale = 1.0 / math.sqrt(width)
    owned = iota((n, total), 0) == iota((n, total), 1) // slots
    fold = [
        jnp.concatenate(
            [
                hot(iota((total, 128), 1) == (3 * ls + part) * slots + iota((total, 128), 0) % slots)
                for part in range(3)
            ],
            axis=0,
        )
        for ls in range(own)
    ]

    whole(recv.at[pl.ds(0, n - 1)], row_sem.at[0], row_sem.at[2]).wait_recv()
    def pick_copy(peer):
        return remote(
            pick.at[peer], recv_pick.at[me], pick_sem.at[0], pick_sem.at[1], peer, 0
        )

    each_chip(lambda peer: pick_copy(peer).start(), 0)
    recv_pick[me] = pick[me]

    told = None
    table_copy.wait_recv()
    whole(recv.at[pl.ds(n, n)], row_sem.at[1], row_sem.at[3]).wait_recv()
    for ls in range(own):
        scores[ls] = dot_nt(
            jnp.concatenate([desc[own * core + ls], table[ls]], axis=1),
            jnp.concatenate(
                [recv[x * n : (x + 1) * n, ls].reshape(total, half) for x in range(2)], axis=1
            ),
        )

        def chunk(i, carry):
            top, picked, claimed = carry
            at = pl.ds(pl.multiple_of(i * step, step), step)
            value = scores[ls, at, :]
            masked = value + bias[ls, at, :]
            claim = jnp.max(masked, axis=1, keepdims=True)
            chosen = code(iota((step, total), 0) + i * step, cands).astype(F32) == picks[ls : ls + 1]

            def least(v):
                return jnp.max(v.reshape(step // 8, 8, total), axis=0)

            return (
                jnp.maximum(top, least(masked)),
                jnp.maximum(picked, least(jnp.where(chosen, value, NEG))),
                jnp.maximum(claimed, least(jnp.where(chosen, claim, NEG))),
            )

        start = jnp.full((8, total), NEG, F32)
        top, picked, claimed = [
            jnp.max(v, axis=0, keepdims=True)
            for v in lax.fori_loop(0, cands // step, chunk, (start, start, start), unroll=True)
        ]

        def quality(v):
            v = v * scale
            return 1.0 + jnp.maximum(v, 0.0) + jnp.log(1.0 + jnp.exp(-jnp.abs(v)))

        mine = quality(picked)
        share = mine / (mine + quality(claimed))
        high = share.astype(BF16).astype(F32)
        top = jnp.where(top > NEG * 0.5, top * scale, 0.0)
        spread = jnp.concatenate(
            [jnp.where(owned, jnp.broadcast_to(v, (n, total)), 0.0) for v in (high, share - high, top)],
            axis=1,
        ).astype(BF16)
        term = dot(spread, fold[ls])
        told = term if told is None else told + term
    res[...] = told.reshape(n, 1, 128)
    each_peer(
        lambda peer, x: remote(
            res.at[peer], recv_res.at[x * n + me], res_sem.at[0], res_sem.at[1], peer, x
        ).start()
    )
    recv_res[me] = res[me]
    each_chip(lambda peer: pick_copy(peer).start(), 1)

    kind = iota((128, half + halos), 0) // slots % 3
    first = iota((128, half + halos), 1) < half
    merge = hot((first & (kind < 2)) | (~first & (kind == 2)))
    eye = iota((halos, halos), 0) == iota((halos, halos), 1)
    whole(recv_pick.at[pl.ds(0, n - 1)], pick_sem.at[0], pick_sem.at[1]).wait_recv()
    rows = [
        dot(back[i][2], recv_pick[:, 2 * ls + x].reshape(total, half)) for i, (x, ls) in enumerate(order)
    ]
    whole(recv_res.at[pl.ds(0, 2 * n - 1)], res_sem.at[0], res_sem.at[1]).wait_recv()
    spread = [
        dot(
            jnp.concatenate([back[x * own + ls][0] for ls in range(own)], axis=0),
            recv_res[x * n : (x + 1) * n].reshape(n, 128).astype(BF16),
        )
        for x in range(2)
    ]
    spread = jnp.where(
        jnp.concatenate([v[1] for v in back], axis=0), jnp.concatenate(spread, axis=0), 0.0
    ).astype(BF16)
    spread = dot(spread, merge)
    tops = []
    for i, (x, ls) in enumerate(order):
        s = own * core_of(x) + ls
        share = spread[i * halos : (i + 1) * halos, :half]
        phantom[s] = ((1.0 - share) * halo[s].astype(F32) + share * rows[i]).astype(BF16)
        tops.append(
            jnp.sum(jnp.where(eye, spread[i * halos : (i + 1) * halos, half:], 0.0), axis=0, keepdims=True)
        )
    first, second = jnp.concatenate(tops[:own], axis=0), jnp.concatenate(tops[own:], axis=0)
    even = core == 0
    best[...] = jnp.concatenate(
        [jnp.where(even, first, second), jnp.where(even, second, first)], axis=0
    ).astype(BF16)

    table_copy.wait_send()
    whole(send_want.at[pl.ds(0, n - 1)], want_sem.at[0], want_sem.at[1]).wait_send()
    whole(send_meta.at[pl.ds(0, n - 1)], meta_sem.at[0], meta_sem.at[1]).wait_send()
    whole(send.at[pl.ds(0, n - 1)], row_sem.at[0], row_sem.at[2]).wait_send()
    whole(send.at[pl.ds(0, n)], row_sem.at[1], row_sem.at[3]).wait_send()
    whole(pick.at[pl.ds(0, n - 1)], pick_sem.at[0], pick_sem.at[1]).wait_send()
    whole(recv_res.at[pl.ds(0, 2 * n - 1)], res_sem.at[0], res_sem.at[1]).wait_send()


def hand_over(phantom_in, best_in, phantom, best):
    phantom[...] = phantom_in[...]
    best[...] = best_in[...]


def body(n, halo_rows, unmatched, owner_id, cand_index, lengths, choice_index, desc_rows):
    snaps, halos, half = halo_rows.shape
    cands = desc_rows.shape[1]
    own = snaps // 2
    slots = max(2 * halos // n, 16)
    total = n * slots
    dma = pltpu.SemaphoreType.DMA
    results = pl.pallas_call(
        functools.partial(kernel, n, slots, 2 * half),
        out_shape=(
            pltpu.VMEM((snaps, halos, half), BF16),
            pltpu.VMEM((snaps, halos), BF16),
        ),
        in_specs=[pl.BlockSpec(memory_space=pl.ANY)] * 7,
        out_specs=(pl.BlockSpec(memory_space=pltpu.VMEM),) * 2,
        scratch_shapes=[
            pltpu.VMEM(halo_rows.shape, BF16),
            pltpu.VMEM(unmatched.shape, jnp.int32),
            pltpu.VMEM((snaps, 1, halos), jnp.int32),
            pltpu.VMEM((snaps, cand_index.shape[2], halos), jnp.int32),
            pltpu.VMEM(lengths.shape, jnp.int32),
            pltpu.VMEM(choice_index.shape, jnp.int32),
            pltpu.VMEM((snaps, cands, half), BF16),
            pltpu.VMEM((own, cands, half), BF16),
            pltpu.VMEM((2 * n, own, slots, half), BF16),
            pltpu.VMEM((2 * n, own, slots, half), BF16),
            pltpu.VMEM((n, 1, 128), F32),
            pltpu.VMEM((n, 1, 128), F32),
            pltpu.VMEM((n, slots // PARTS, 128), BF16),
            pltpu.VMEM((n, slots // PARTS, 128), BF16),
            pltpu.VMEM((own, cands, total), F32),
            pltpu.VMEM((own, cands, total), F32),
            pltpu.VMEM((n, snaps, slots, half), BF16),
            pltpu.VMEM((n, snaps, slots, half), BF16),
            pltpu.VMEM((n, 1, 128), F32),
            pltpu.VMEM((2 * n, 1, 128), F32),
            dma((4,)), dma((2,)), dma((2,)), dma((2,)), dma((2,)), dma((2,)), dma((7,)),
        ],
        compiler_params=pltpu.CompilerParams(collective_id=0, has_side_effects=True),
    )(
        halo_rows,
        unmatched,
        jnp.swapaxes(owner_id, 1, 2),
        jnp.swapaxes(cand_index, 1, 2),
        lengths,
        choice_index,
        desc_rows,
    )
    shapes = tuple(jax.ShapeDtypeStruct(v.shape, v.dtype) for v in results)
    return pl.pallas_call(
        hand_over,
        out_shape=shapes,
        in_specs=[pl.BlockSpec(memory_space=pltpu.VMEM)] * 2,
        out_specs=(pl.BlockSpec(memory_space=pltpu.VMEM),) * 2,
    )(*[pltpu.with_memory_space_constraint(v, pltpu.VMEM) for v in results])


def solution(mesh):
    in_specs = (
        P(None, "space", "rep"),
        P(None, "space"),
        P(None, "space", None),
        P(None, "space", None),
        P(None, "space"),
        P(None, "space"),
        P(None, "space", "rep"),
    )
    out_specs = (P(None, "space", "rep"), P(None, "space"))
    return jax.shard_map(
        functools.partial(body, mesh.shape["space"]),
        mesh=mesh, in_specs=in_specs, out_specs=out_specs, check_vma=False,
    )
```

```python
import functools
import math

import jax
import jax.numpy as jnp
from jax import lax
from jax.experimental import pallas as pl
from jax.experimental.pallas import tpu as pltpu
from jax.sharding import PartitionSpec as P

MESH = pl.DeviceIdType.MESH
F32 = jnp.float32
BF16 = jnp.bfloat16
NEG = -1e30
PARTS = 4
NT = (((1,), (1,)), ((), ()))


def iota(shape, dim):
    return lax.broadcasted_iota(jnp.int32, shape, dim)


def dot(a, b):
    return jnp.dot(a, b, preferred_element_type=F32)


def dot_nt(a, b):
    return lax.dot_general(a, b, NT, preferred_element_type=F32)


def hot(mask):
    return jnp.where(mask, 1.0, 0.0).astype(BF16)


def code(index, cands):
    return index - cands // 2 + jnp.where(index >= cands // 2, 1, 0)


def kernel(
    n, slots, width,
    halo_in, unmatched_in, owner_in, cand_in, lengths_in, choice_in, desc_in,
    phantom, best,
    halo, unmatched, owner, cand, lengths, choice, desc, table,
    send, recv, send_want, recv_want, send_meta, recv_meta, scores, bias, pick, recv_pick, res, recv_res,
    row_sem, want_sem, meta_sem, pick_sem, res_sem, table_sem, load_sem,
):
    me, core = lax.axis_index("space"), lax.axis_index("rep")
    snaps, halos, half = halo.shape
    k_count = cand.shape[1]
    cands = desc.shape[1]
    own = snaps // 2
    total = n * slots
    qs = slots // PARTS

    def core_of(x):
        return 1 - core if x else core

    def remote(src, dst, ss, rs, peer, x):
        return pltpu.make_async_remote_copy(
            src_ref=src, dst_ref=dst, send_sem=ss, recv_sem=rs,
            device_id=(peer, core_of(x)), device_id_type=MESH,
        )

    def whole(ref, ss, rs):
        return remote(ref, ref, ss, rs, me, 1)

    def each_chip(f, part=None):
        if n % 4 or n > 32:
            low, high = {None: (1, n), 0: (1, n // 2), 1: (n // 2, n)}[part]

            @pl.loop(low, high)
            def _(d):
                peer = me + d
                f(jnp.where(peer >= n, peer - n, peer))

            return
        blocks = [*range(1, n // 4), 0]
        if part is not None:
            blocks = blocks[n // 8 :] if part else blocks[: n // 8]
        block, place = me // 4, lax.rem(me, 4)
        for d in blocks:
            to = block + d
            to = jnp.where(to >= n // 4, to - n // 4, to) * 4
            for q in (3, 1, 2, 0):
                if d or q:
                    f(to + jnp.bitwise_xor(place, q))

    def each_peer(f):
        def both(peer):
            f(peer, 0)
            f(peer, 1)

        each_chip(both)
        f(me, 1)

    barrier = pltpu.get_barrier_semaphore()
    each_peer(
        lambda peer, x: pl.semaphore_signal(
            barrier, inc=1, device_id=(peer, core_of(x)), device_id_type=MESH
        ),
    )
    loads = [
        pltpu.make_async_copy(src, dst, load_sem.at[i])
        for i, (src, dst) in enumerate(
            [
                (owner_in, owner), (unmatched_in, unmatched), (cand_in, cand),
                (lengths_in, lengths), (choice_in, choice), (halo_in, halo), (desc_in, desc),
            ]
        )
    ]
    for load in loads:
        load.start()
    for load in loads[:5]:
        load.wait()

    order = [(x, ls) for x in range(2) for ls in range(own)]
    named = [iota((n, halos), 0) == owner[own * core_of(x) + ls] for x, ls in order]
    onehot = hot(jnp.concatenate(named, axis=0))
    before = dot(onehot, hot(iota((halos, halos), 0) < iota((halos, halos), 1)))
    route = []
    for i, (x, ls) in enumerate(order):
        s = own * core_of(x) + ls
        rank = jnp.sum(
            jnp.where(named[i], before[i * n : (i + 1) * n], 0.0), axis=0, keepdims=True
        ).astype(jnp.int32)
        live = unmatched[pl.ds(s, 1), :] == 1
        dest = owner[s]
        route.append((dest, rank, jnp.where(live, dest * slots + rank, -1), live))

    k_ids = iota((k_count, halos), 0)
    wants, coded = [], []
    for i, (x, ls) in enumerate(order):
        s = own * core_of(x) + ls
        _, rank, _, live = route[i]
        coded.append(code(cand[s], cands))
        taken = jnp.sum(
            jnp.where(k_ids == choice[pl.ds(s, 1), :], coded[i], 0), axis=0, keepdims=True
        )
        wants.append(jnp.where(live & (iota((slots, halos), 0) == rank), taken, 0).astype(F32))
    blank = jnp.zeros((slots, halos), F32)
    table_of = [
        jnp.concatenate([wants[i] if i == j else blank for i in range(snaps)], axis=1) for j in range(snaps)
    ]
    table_of.append(jnp.zeros((128 - snaps * slots, snaps * halos), F32))
    told = dot_nt(
        jnp.concatenate([hot(v) for v in named], axis=1), jnp.concatenate(table_of, axis=0).astype(BF16)
    )
    send_want[...] = told.reshape(n, 1, 128)

    blocks, rows = [], []
    for ls in range(own):
        dest, rank, _, live = route[ls]
        listed = jnp.where(k_ids < lengths[pl.ds(own * core + ls, 1), :], coded[ls], 0).astype(F32)
        none = jnp.zeros((k_count, halos), F32)
        blocks.append(jnp.concatenate([listed if i == ls else none for i in range(own)], axis=0))
        rows.append(
            [
                jnp.where(live & (rank >= g * qs) & (rank < (g + 1) * qs), dest * qs + rank - g * qs, -1)
                for g in range(PARTS)
            ]
        )
    block = jnp.concatenate(blocks, axis=1).astype(BF16)
    blank = jnp.zeros_like(block)
    meta = sum(
        dot_nt(
            jnp.concatenate([hot(iota((n * qs, halos), 0) == r[g]) for r in rows], axis=1),
            jnp.concatenate([block if i == g else blank for i in range(PARTS)], axis=0),
        )
        for g in range(PARTS)
    )
    send_meta[...] = meta.astype(BF16).reshape(n, qs, 128)

    loads[5].wait()
    for i, (x, ls) in enumerate(order):
        place = hot(iota((total, halos), 0) == route[i][2])
        packed = dot(place, halo[own * core_of(x) + ls]).astype(BF16)
        send[x * n : (x + 1) * n, ls] = packed.reshape(n, slots, half)

    pl.semaphore_wait(barrier, 2 * n - 1)

    each_chip(
        lambda peer: remote(
            send_want.at[peer], recv_want.at[me], want_sem.at[0], want_sem.at[1], peer, 0
        ).start()
    )
    each_chip(
        lambda peer: remote(
            send_meta.at[peer], recv_meta.at[me], meta_sem.at[0], meta_sem.at[1], peer, 0
        ).start()
    )
    def row_copy(peer, x):
        return remote(
            send.at[x * n + peer], recv.at[x * n + me], row_sem.at[x], row_sem.at[2 + x], peer, x
        )

    each_chip(lambda peer: row_copy(peer, 0).start())
    each_chip(lambda peer: row_copy(peer, 1).start())
    row_copy(me, 1).start()
    table_copy = remote(
        desc_in.at[pl.ds(own * core_of(1), own)], table, table_sem.at[0], table_sem.at[1], me, 1
    )
    table_copy.start()
    recv_want[me] = send_want[me]
    recv_meta[me] = send_meta[me]
    recv[me] = send[me]

    lines = [v.astype(F32) for dest, rank, target, live in route for v in (dest, jnp.where(live, rank, -128), target)]
    lines = jnp.concatenate(lines + [jnp.zeros((128 - len(lines), halos), F32)], axis=0).T
    back = []
    lane = iota((halos, 128), 1).astype(F32)
    for i in range(snaps):
        dest, rank, target = [lines[:, 3 * i + j : 3 * i + j + 1] for j in range(3)]
        back.append(
            (
                hot(iota((halos, n), 1).astype(F32) == dest),
                functools.reduce(
                    jnp.logical_or, [lane == rank + (3 * (i % own) + part) * slots for part in range(3)]
                ),
                hot(iota((halos, total), 1).astype(F32) == target),
            )
        )
    entry = iota((n * qs, total), 0)
    column = iota((n * qs, total), 1)
    inside = column % slots
    unpack = [
        hot((entry == (column // slots) * qs + inside - g * qs) & (inside // qs == g)) for g in range(PARTS)
    ]
    loads[6].wait()

    ids = code(iota((total, cands), 1), cands).astype(F32)
    from_chip = hot(iota((total, n), 1) == iota((total, n), 0) // slots)
    its_slot = iota((total, 128), 1) % slots == iota((total, 128), 0) % slots
    part = [hot(iota((128, 128), 0) // slots == i) for i in range(snaps)]

    whole(recv_want.at[pl.ds(0, n - 1)], want_sem.at[0], want_sem.at[1]).wait_recv()
    wanted = dot(from_chip, recv_want[...].reshape(n, 128).astype(BF16))
    wanted = jnp.where(its_slot, wanted, 0.0).astype(BF16)
    picks = dot_nt(hot(iota((8, 128), 1) // slots == iota((8, 128), 0)), wanted)
    for i, (x, ls) in enumerate(order):
        at = jnp.concatenate([dot(wanted, part[i])] * (cands // 128), axis=1)
        chosen = dot(hot(at == ids), desc[own * core_of(x) + ls]).astype(BF16)
        pick[:, 2 * ls + x] = chosen.reshape(n, slots, half)
    step = 64
    whole(recv_meta.at[pl.ds(0, n - 1)], meta_sem.at[0], meta_sem.at[1]).wait_recv()
    arrived = recv_meta[...].reshape(n * qs, 128).astype(F32).T.astype(BF16)
    for ls in range(own):
        lists = sum(
            dot(arrived[(g * own + ls) * k_count : (g * own + ls + 1) * k_count], unpack[g])
            for g in range(PARTS)
        )
        listed = lists.astype(jnp.int32)
        at = listed + cands // 2 - jnp.where(listed > 0, 1, 0)
        flag = jnp.where(listed == 0, 0, jnp.left_shift(1, at & 31))
        at = at >> 5
        words = jnp.zeros((cands // 32, total), jnp.int32)
        for k in range(k_count):
            words = words | jnp.where(iota((cands // 32, total), 0) == at[k : k + 1], flag[k : k + 1], 0)
        bit = jnp.left_shift(1, iota((32, total), 0))
        for w in range(cands // 32):
            bias[ls, 32 * w : 32 * w + 32, :] = jnp.where((words[w : w + 1] & bit) != 0, 0.0, NEG)

    scale = 1.0 / math.sqrt(width)
    owned = iota((n, total), 0) == iota((n, total), 1) // slots
    fold = [
        jnp.concatenate(
            [
                hot(iota((total, 128), 1) == (3 * ls + part) * slots + iota((total, 128), 0) % slots)
                for part in range(3)
            ],
            axis=0,
        )
        for ls in range(own)
    ]

    whole(recv.at[pl.ds(0, n - 1)], row_sem.at[0], row_sem.at[2]).wait_recv()
    def pick_copy(peer):
        return remote(
            pick.at[peer], recv_pick.at[me], pick_sem.at[0], pick_sem.at[1], peer, 0
        )

    def other_pick(peer):
        @pl.when(peer != 0)
        def _():
            pick_copy(peer).start()

    @pl.when(me != 0)
    def _():
        pick_copy(0).start()

    each_chip(other_pick, 0)
    recv_pick[me] = pick[me]

    told = None
    table_copy.wait_recv()
    whole(recv.at[pl.ds(n, n)], row_sem.at[1], row_sem.at[3]).wait_recv()
    for ls in range(own):
        scores[ls] = dot_nt(
            jnp.concatenate([desc[own * core + ls], table[ls]], axis=1),
            jnp.concatenate(
                [recv[x * n : (x + 1) * n, ls].reshape(total, half) for x in range(2)], axis=1
            ),
        )

        def chunk(i, carry):
            top, picked, claimed = carry
            at = pl.ds(pl.multiple_of(i * step, step), step)
            value = scores[ls, at, :]
            masked = value + bias[ls, at, :]
            claim = jnp.max(masked, axis=1, keepdims=True)
            chosen = code(iota((step, total), 0) + i * step, cands).astype(F32) == picks[ls : ls + 1]

            def least(v):
                return jnp.max(v.reshape(step // 8, 8, total), axis=0)

            return (
                jnp.maximum(top, least(masked)),
                jnp.maximum(picked, least(jnp.where(chosen, value, NEG))),
                jnp.maximum(claimed, least(jnp.where(chosen, claim, NEG))),
            )

        start = jnp.full((8, total), NEG, F32)
        top, picked, claimed = [
            jnp.max(v, axis=0, keepdims=True)
            for v in lax.fori_loop(0, cands // step, chunk, (start, start, start), unroll=True)
        ]

        def quality(v):
            v = v * scale
            return 1.0 + jnp.maximum(v, 0.0) + jnp.log(1.0 + jnp.exp(-jnp.abs(v)))

        mine = quality(picked)
        share = mine / (mine + quality(claimed))
        high = share.astype(BF16).astype(F32)
        top = jnp.where(top > NEG * 0.5, top * scale, 0.0)
        spread = jnp.concatenate(
            [jnp.where(owned, jnp.broadcast_to(v, (n, total)), 0.0) for v in (high, share - high, top)],
            axis=1,
        ).astype(BF16)
        term = dot(spread, fold[ls])
        told = term if told is None else told + term
    res[...] = told.reshape(n, 1, 128)
    each_peer(
        lambda peer, x: remote(
            res.at[peer], recv_res.at[x * n + me], res_sem.at[0], res_sem.at[1], peer, x
        ).start()
    )
    recv_res[me] = res[me]
    each_chip(other_pick, 1)

    kind = iota((128, half + halos), 0) // slots % 3
    first = iota((128, half + halos), 1) < half
    merge = hot((first & (kind < 2)) | (~first & (kind == 2)))
    eye = iota((halos, halos), 0) == iota((halos, halos), 1)
    whole(recv_pick.at[pl.ds(0, n - 1)], pick_sem.at[0], pick_sem.at[1]).wait_recv()
    rows = [
        dot(back[i][2], recv_pick[:, 2 * ls + x].reshape(total, half)) for i, (x, ls) in enumerate(order)
    ]
    whole(recv_res.at[pl.ds(0, 2 * n - 1)], res_sem.at[0], res_sem.at[1]).wait_recv()
    spread = [
        dot(
            jnp.concatenate([back[x * own + ls][0] for ls in range(own)], axis=0),
            recv_res[x * n : (x + 1) * n].reshape(n, 128).astype(BF16),
        )
        for x in range(2)
    ]
    spread = jnp.where(
        jnp.concatenate([v[1] for v in back], axis=0), jnp.concatenate(spread, axis=0), 0.0
    ).astype(BF16)
    spread = dot(spread, merge)
    tops = []
    for i, (x, ls) in enumerate(order):
        s = own * core_of(x) + ls
        share = spread[i * halos : (i + 1) * halos, :half]
        phantom[s] = ((1.0 - share) * halo[s].astype(F32) + share * rows[i]).astype(BF16)
        tops.append(
            jnp.sum(jnp.where(eye, spread[i * halos : (i + 1) * halos, half:], 0.0), axis=0, keepdims=True)
        )
    first, second = jnp.concatenate(tops[:own], axis=0), jnp.concatenate(tops[own:], axis=0)
    even = core == 0
    best[...] = jnp.concatenate(
        [jnp.where(even, first, second), jnp.where(even, second, first)], axis=0
    ).astype(BF16)

    table_copy.wait_send()
    whole(send_want.at[pl.ds(0, n - 1)], want_sem.at[0], want_sem.at[1]).wait_send()
    whole(send_meta.at[pl.ds(0, n - 1)], meta_sem.at[0], meta_sem.at[1]).wait_send()
    whole(send.at[pl.ds(0, n - 1)], row_sem.at[0], row_sem.at[2]).wait_send()
    whole(send.at[pl.ds(0, n)], row_sem.at[1], row_sem.at[3]).wait_send()
    whole(pick.at[pl.ds(0, n - 1)], pick_sem.at[0], pick_sem.at[1]).wait_send()
    whole(recv_res.at[pl.ds(0, 2 * n - 1)], res_sem.at[0], res_sem.at[1]).wait_send()


def hand_over(phantom_in, best_in, phantom, best):
    phantom[...] = phantom_in[...]
    best[...] = best_in[...]


def body(n, halo_rows, unmatched, owner_id, cand_index, lengths, choice_index, desc_rows):
    snaps, halos, half = halo_rows.shape
    cands = desc_rows.shape[1]
    own = snaps // 2
    slots = max(2 * halos // n, 16)
    total = n * slots
    dma = pltpu.SemaphoreType.DMA
    results = pl.pallas_call(
        functools.partial(kernel, n, slots, 2 * half),
        out_shape=(
            pltpu.VMEM((snaps, halos, half), BF16),
            pltpu.VMEM((snaps, halos), BF16),
        ),
        in_specs=[pl.BlockSpec(memory_space=pl.ANY)] * 7,
        out_specs=(pl.BlockSpec(memory_space=pltpu.VMEM),) * 2,
        scratch_shapes=[
            pltpu.VMEM(halo_rows.shape, BF16),
            pltpu.VMEM(unmatched.shape, jnp.int32),
            pltpu.VMEM((snaps, 1, halos), jnp.int32),
            pltpu.VMEM((snaps, cand_index.shape[2], halos), jnp.int32),
            pltpu.VMEM(lengths.shape, jnp.int32),
            pltpu.VMEM(choice_index.shape, jnp.int32),
            pltpu.VMEM((snaps, cands, half), BF16),
            pltpu.VMEM((own, cands, half), BF16),
            pltpu.VMEM((2 * n, own, slots, half), BF16),
            pltpu.VMEM((2 * n, own, slots, half), BF16),
            pltpu.VMEM((n, 1, 128), F32),
            pltpu.VMEM((n, 1, 128), F32),
            pltpu.VMEM((n, slots // PARTS, 128), BF16),
            pltpu.VMEM((n, slots // PARTS, 128), BF16),
            pltpu.VMEM((own, cands, total), F32),
            pltpu.VMEM((own, cands, total), F32),
            pltpu.VMEM((n, snaps, slots, half), BF16),
            pltpu.VMEM((n, snaps, slots, half), BF16),
            pltpu.VMEM((n, 1, 128), F32),
            pltpu.VMEM((2 * n, 1, 128), F32),
            dma((4,)), dma((2,)), dma((2,)), dma((2,)), dma((2,)), dma((2,)), dma((7,)),
        ],
        compiler_params=pltpu.CompilerParams(collective_id=0, has_side_effects=True),
    )(
        halo_rows,
        unmatched,
        jnp.swapaxes(owner_id, 1, 2),
        jnp.swapaxes(cand_index, 1, 2),
        lengths,
        choice_index,
        desc_rows,
    )
    shapes = tuple(jax.ShapeDtypeStruct(v.shape, v.dtype) for v in results)
    return pl.pallas_call(
        hand_over,
        out_shape=shapes,
        in_specs=[pl.BlockSpec(memory_space=pltpu.VMEM)] * 2,
        out_specs=(pl.BlockSpec(memory_space=pltpu.VMEM),) * 2,
    )(*[pltpu.with_memory_space_constraint(v, pltpu.VMEM) for v in results])


def solution(mesh):
    in_specs = (
        P(None, "space", "rep"),
        P(None, "space"),
        P(None, "space", None),
        P(None, "space", None),
        P(None, "space"),
        P(None, "space"),
        P(None, "space", "rep"),
    )
    out_specs = (P(None, "space", "rep"), P(None, "space"))
    return jax.shard_map(
        functools.partial(body, mesh.shape["space"]),
        mesh=mesh, in_specs=in_specs, out_specs=out_specs, check_vma=False,
    )
```
